32 devices in a mesh: row: 8 (over z, core), col: 4 (over y, x).
Axes of the slice: x: 2, y: 2, z: 4, core: 2. Of those that a mesh axis runs over, the one named last changes fastest.
Arguments:
- u_start: float32 [128, 131072], P('col', 'row'), may hold values from -24 to 24
- v_start: float32 [128, 65536], P('row', 'col'), may hold values from -24 to 24
- keep_u: float32 [128, 40], replicated, may hold values from -1 to 1, as said below
- keep_v: float32 [128, 40], replicated, may hold values from -1 to 1, as said below
- v_next: float32 [65536], P(('col', 'row')), may hold values from -96 to 96
- tile_blocks: bfloat16 [2048, 256, 256], P(('row', 'col')), may hold values from -0.375 to 0.375
- tile_rows: int32 [2048], P(('row', 'col')), may hold values from 0 to 63
- tile_cols: int32 [2048], P(('row', 'col')), may hold values from 0 to 63
- tile_count: int32 [32], P(('row', 'col')), may hold values from 32 to 64
Outputs:
- u_basis: float32 [42, 131072], P(None, ('row', 'col'))
- v_basis: float32 [43, 65536], P(None, ('col', 'row'))
- bidiagonal: float32 [2, 2], replicated
The draws below stay inside these ranges and needn't reach their ends.
Inputs may be any that keep to these rules, and one draw needn't show every extreme that they name: `tile_rows`: tile row within the device's row group. `tile_cols`: tile column within the device's column group. `tile_count`: slots at this index and beyond hold no tile. `keep_u`: the columns are orthonormal. `keep_v`: the columns are orthonormal.
All inputs are finite; a program needn't handle non-finite values.
Results may differ from the reference program's by a relative error of at most 0.00155.
Values may be sent and summed in bfloat16 or wider, within the bound.
A program may use at most 64 MiB of HBM per device.

```python
import jax
import jax.numpy as jnp
from jax import lax

BASIS = 128
KEEP = 40
TILE = 256
STEPS = 2
RB = 64
CB = 64
TILES_DEV = 64
M = 131072
N = 65536
TILES = 2048
N_COL = 4
DEVICES = 32


def basis_rows_draw(key, count, length):
    raw = jax.random.normal(jax.random.fold_in(key, 1), (length, count), jnp.float32)
    factor, upper = jnp.linalg.qr(raw)
    rows = factor.T * jnp.sqrt(jnp.float32(length))
    along = jnp.arange(length, dtype=jnp.float32) / jnp.float32(length)
    inner = along * jnp.float32(N_COL) - jnp.floor(along * jnp.float32(N_COL))
    weight = (1.0 + 2.0 * along) * (1.0 + 2.0 * inner)
    row_scale = jax.random.uniform(jax.random.fold_in(key, 2), (count, 1), jnp.float32, 0.7, 1.3)
    rows = rows * weight[None, :]
    rows = rows / jnp.sqrt(jnp.mean(rows * rows, axis=1, keepdims=True))
    rows = rows * row_scale
    return jnp.clip(rows, -24.0, 24.0).astype(jnp.float32)


def columns_draw(key, count, width):
    raw = jax.random.normal(key, (count, width), jnp.float32)
    factor, upper = jnp.linalg.qr(raw)
    return factor.astype(jnp.float32)


def draw_u_start(key, part):
    return basis_rows_draw(jax.random.fold_in(key, 11), BASIS, M)


def draw_v_start(key, part):
    return basis_rows_draw(jax.random.fold_in(key, 23), BASIS, N)


def draw_keep_u(key, part):
    return columns_draw(jax.random.fold_in(key, 37), BASIS, KEEP)


def draw_keep_v(key, part):
    return columns_draw(jax.random.fold_in(key, 41), BASIS, KEEP)


def draw_v_next(key, part):
    rows = basis_rows_draw(jax.random.fold_in(key, 23), BASIS, N)
    mixing = 0.5 * jax.random.normal(jax.random.fold_in(key, 59), (BASIS,), jnp.float32)
    noise = jax.random.normal(jax.random.fold_in(key, 61), (N,), jnp.float32)
    mixed = noise + jnp.dot(mixing, rows, precision=jax.lax.Precision.HIGHEST)
    return jnp.clip(mixed, -96.0, 96.0).astype(jnp.float32)


def plant(entries, stream_key, low, high):
    spot = [jax.random.randint(jax.random.fold_in(stream_key, axis), (), 0, length) for axis, length in enumerate(entries.shape)]
    longest = entries.shape.index(max(entries.shape))
    neighbour = spot[:longest] + [(spot[longest] + 1) % entries.shape[longest]] + spot[longest + 1:]
    return entries.at[tuple(spot)].set(low).at[tuple(neighbour)].set(high)


def level_of(own_key, extent, pieces, low, largest):
    def one(position, blocks):
        heights = jax.random.uniform(jax.random.fold_in(jax.random.fold_in(own_key, 6), position), (blocks,), jnp.float32, low / len(pieces), largest / len(pieces))
        return jnp.repeat(jnp.exp(heights), extent[position] // blocks).reshape((-1,) + (1,) * (len(extent) - position - 1))

    level = one(*pieces[0])
    for cut in pieces[1:]:
        level = level * one(*cut)
    return level


def scatter_about(rng, shape, deviation, limit, shards=(), kind=jnp.bfloat16):
    gain = level_of(rng, shape, shards, -0.22, 0.18) if shards else 1.0
    array = jax.random.normal(rng, shape, jnp.float32) * deviation * gain
    return jnp.minimum(jnp.maximum(array, -limit), limit).astype(kind)


def setup_inputs(seed: int = 0) -> dict:
    splits = jax.random.split(jax.random.key(seed), 10)
    u_start = draw_u_start(jax.random.fold_in(splits[9], 71), 0)
    v_start = draw_v_start(jax.random.fold_in(splits[9], 71), 0)
    keep_u = draw_keep_u(jax.random.fold_in(splits[9], 71), 0)
    keep_v = draw_keep_v(jax.random.fold_in(splits[9], 71), 0)
    v_next = draw_v_next(jax.random.fold_in(splits[9], 71), 0)
    tile_blocks = scatter_about(splits[5], (TILES, TILE, TILE), TILE ** -0.5, 0.375, ((0, 32),))
    tile_rows = plant(jax.random.randint(splits[6], (TILES,), 0, RB), jax.random.fold_in(splits[6], 1), 0, RB - 1).astype(jnp.int32)
    tile_cols = plant(jax.random.randint(splits[7], (TILES,), 0, CB), jax.random.fold_in(splits[7], 1), 0, CB - 1).astype(jnp.int32)
    tile_count = plant(jax.random.randint(splits[8], (DEVICES,), TILES_DEV // 2, TILES_DEV + 1), jax.random.fold_in(splits[8], 1), TILES_DEV // 2, TILES_DEV).astype(jnp.int32)
    return {"u_start": u_start, "v_start": v_start, "keep_u": keep_u, "keep_v": keep_v, "v_next": v_next, "tile_blocks": tile_blocks, "tile_rows": tile_rows, "tile_cols": tile_cols, "tile_count": tile_count}


HIGH = lax.Precision.HIGHEST

def tile_product(tile_blocks, tile_rows, tile_cols, tile_count, vector, forward_pass):
    rounded = lax.optimization_barrier(vector.astype(jnp.bfloat16)).astype(jnp.float32)
    if forward_pass:
        blocks = rounded.reshape(N // TILE, TILE)
        segments = M // TILE
    else:
        blocks = rounded.reshape(M // TILE, TILE)
        segments = N // TILE
    grouped = tile_blocks.reshape(DEVICES, TILES_DEV, TILE, TILE)
    row_slots = tile_rows.reshape(DEVICES, TILES_DEV)
    col_slots = tile_cols.reshape(DEVICES, TILES_DEV)

    def per_device(device):
        row_group = device // N_COL
        col_group = device % N_COL
        tile_float = lax.dynamic_index_in_dim(grouped, device, 0, keepdims=False).astype(jnp.float32)
        local_rows = lax.dynamic_index_in_dim(row_slots, device, 0, keepdims=False)
        local_cols = lax.dynamic_index_in_dim(col_slots, device, 0, keepdims=False)
        active = (jnp.arange(TILES_DEV, dtype=jnp.int32) < tile_count[device]).astype(jnp.float32)
        row_index = (row_group * RB + local_rows).astype(jnp.int32)
        col_index = (col_group * CB + local_cols).astype(jnp.int32)
        if forward_pass:
            picked = blocks[col_index]
            outputs = jnp.einsum('tij,tj->ti', tile_float, picked, precision=HIGH)
            target = row_index
        else:
            picked = blocks[row_index]
            outputs = jnp.einsum('tij,ti->tj', tile_float, picked, precision=HIGH)
            target = col_index
        return (outputs * active[:, None], target)
    outputs, target = lax.map(per_device, jnp.arange(DEVICES, dtype=jnp.int32))
    summed = jax.ops.segment_sum(outputs.reshape(-1, TILE), target.reshape(-1), num_segments=segments)
    return summed.reshape(-1)

def orthonormal(basis_rows, vector):
    length = vector.shape[0]
    first_coef = jnp.dot(basis_rows, vector, precision=HIGH) / length
    once_clean = vector - jnp.dot(first_coef, basis_rows, precision=HIGH)
    second_coef = jnp.dot(basis_rows, once_clean, precision=HIGH) / length
    twice_clean = once_clean - jnp.dot(second_coef, basis_rows, precision=HIGH)
    scale_now = jnp.sqrt(jnp.sum(twice_clean * twice_clean) / length + 1e-06)
    return (twice_clean / scale_now, scale_now)

def reference(u_start, v_start, keep_u, keep_v, v_next, tile_blocks, tile_rows, tile_cols, tile_count):
    u_kept = jnp.dot(keep_u.T, u_start, precision=HIGH)
    v_kept = jnp.dot(keep_v.T, v_start, precision=HIGH)
    first_right, beta_start = orthonormal(v_kept, v_next)
    left_rows = u_kept
    right_rows = jnp.concatenate([v_kept, first_right[None, :]], axis=0)
    current = first_right
    alpha_list = []
    beta_list = []
    for iteration in range(STEPS):
        image = tile_product(tile_blocks, tile_rows, tile_cols, tile_count, current, True)
        left_new, alpha = orthonormal(left_rows, image)
        left_rows = jnp.concatenate([left_rows, left_new[None, :]], axis=0)
        back_image = tile_product(tile_blocks, tile_rows, tile_cols, tile_count, left_new, False)
        current, beta = orthonormal(right_rows, back_image)
        right_rows = jnp.concatenate([right_rows, current[None, :]], axis=0)
        alpha_list.append(alpha)
        beta_list.append(beta)
    bidiagonal = jnp.stack([jnp.stack(alpha_list), jnp.stack(beta_list)])
    return (left_rows, right_rows, bidiagonal)
```

```python
import functools

import jax
import jax.numpy as jnp
from jax import lax
from jax.experimental import pallas as pl
from jax.experimental.pallas import tpu as pltpu
from jax.sharding import PartitionSpec as P

STEPS = 2
HIGH = lax.Precision.HIGHEST
F32 = jnp.float32
BF16 = jnp.bfloat16
I16 = jnp.int16
I32 = jnp.int32
LANE = 128
DIRECT = 32
KNEE = 5.0
FINE = 4800.0
COARSE = 461.0


def encode(x):
    code = x * COARSE + jnp.clip(x, -KNEE, KNEE) * (FINE - COARSE)
    return jnp.round(code).astype(I32).astype(I16)


def decode(code):
    y = code.astype(I32).astype(F32)
    near = jnp.clip(y, -KNEE * FINE, KNEE * FINE)
    return near * (1.0 / FINE) + (y - near) * (1.0 / COARSE)


def partner(me, k, n):
    if n & (n - 1):
        return lax.rem(me + k, n)
    other, bit = 0, 1
    while bit < n:
        digit = lax.rem(lax.div(me, bit), 2)
        other = other + (1 - digit if k & bit else digit) * bit
        bit *= 2
    return other


def kernel(
    row_n, col_n, keep_n, fold, u_hbm, v_hbm, keep_u_hbm, keep_v_hbm, v_next_hbm, tiles_hbm, rows_hbm, cols_hbm,
    count_hbm,
    u_out, v_out, bi_out,
    u_in, v_in, u_code, v_code, u_all, v_all, tiles, keep_u, keep_v, v_first, rows_ref, cols_ref, count_ref,
    u_rows, v_rows, u_vec, v_vec, gram_v_row, gram_v_col, gram_u_col, gram_u_row,
    sum_col, sum_row, sum_all, v_gather, u_gather, u_parts, v_parts, u_recv, v_recv,
    row_pick, col_pick, row_put, col_put, picked, products,
    local_sem, init_u_send, init_u_recv, init_v_send, init_v_recv, send_sem, gram_send, gram_recv,
    sum_col_sem, sum_row_sem, sum_all_sem, vg_sem, ug_sem, ur_sem, vr_sem,
):
    row_me = lax.axis_index("row")
    col_me = lax.axis_index("col")

    def load(index, source, target):
        copy = pltpu.make_async_copy(source, target, local_sem.at[index])
        copy.start()
        return copy

    own_v = load(0, v_hbm, v_in)
    own_u = load(1, u_hbm, u_in)
    own_keep_v = load(2, keep_v_hbm, keep_v)
    own_keep_u = load(3, keep_u_hbm, keep_u)
    own_next = load(4, v_next_hbm, v_first)
    own_places = [load(5, rows_hbm, rows_ref), load(6, cols_hbm, cols_ref), load(7, count_hbm, count_ref)]
    own_t = load(8, tiles_hbm, tiles)

    barrier = pltpu.get_barrier_semaphore()
    for k in range(1, row_n):
        pl.semaphore_signal(barrier, inc=1, device_id={"row": partner(row_me, k, row_n)},
                            device_id_type=pl.DeviceIdType.MESH)
    for k in range(1, col_n):
        pl.semaphore_signal(barrier, inc=1, device_id={"col": partner(col_me, k, col_n)},
                            device_id_type=pl.DeviceIdType.MESH)

    direct = row_n * col_n <= DIRECT
    v_here, u_here = v_all.shape[1], u_all.shape[1]
    u_len, v_len = u_rows.shape[1], v_rows.shape[1]
    u_total = float(u_len * row_n * col_n)
    v_total = float(v_len * row_n * col_n)
    rows_p = u_rows.shape[0]
    keep_p = keep_u.shape[0]
    tile = tiles.shape[1]
    slots = tiles.shape[0]
    u_sub, v_sub = u_len // tile, v_len // tile
    row_blocks, col_blocks = col_n * u_sub, row_n * v_sub
    width = LANE // fold
    part = rows_p // fold

    def send(axis, me, n, src, dst, sends, recvs):
        copies = []
        for k in range(n - 1, 0, -1):
            target = partner(me, k, n)
            copy = pltpu.make_async_remote_copy(
                src_ref=src(target), dst_ref=dst(k), send_sem=sends(k), recv_sem=recvs(k),
                device_id={axis: target}, device_id_type=pl.DeviceIdType.MESH)
            copy.start()
            copies.append(copy)
        return copies

    def finish(copies):
        for copy in copies:
            copy.wait()

    u_rows[...] = jnp.zeros(u_rows.shape, F32)
    v_rows[...] = jnp.zeros(v_rows.shape, F32)
    own_v.wait()
    for p in range(row_n):
        v_code[p] = encode(v_in[:, p * v_len:(p + 1) * v_len])
    own_u.wait()
    for p in range(col_n):
        u_code[p] = encode(u_in[:, p * u_len:(p + 1) * u_len])
    pl.semaphore_wait(barrier, row_n + col_n - 2)
    v_init = send("row", row_me, row_n, lambda p: v_code.at[p], lambda k: v_all.at[row_me],
                  lambda k: init_v_send.at[k], lambda k: init_v_recv.at[k])
    u_init = send("col", col_me, col_n, lambda p: u_code.at[p], lambda k: u_all.at[col_me],
                  lambda k: init_u_send.at[k], lambda k: init_u_recv.at[k])
    v_all[row_me] = v_code[row_me]
    u_all[col_me] = u_code[col_me]

    for copy in own_places:
        copy.wait()
    active = lax.broadcasted_iota(I32, (1, slots), 1) < count_ref[...]

    def hot_of(places, blocks, pick, put):
        hot = jnp.where(
            (lax.broadcasted_iota(I32, (blocks, slots), 0) == places) & active, 1.0, 0.0).astype(BF16)
        eye = (lax.broadcasted_iota(I32, (blocks, blocks), 0)
               == lax.broadcasted_iota(I32, (blocks, blocks), 1))
        pick[...] = lax.dot_general(hot, jnp.where(eye, 1.0, 0.0).astype(BF16), (((0,), (0,)), ((), ())),
                                    preferred_element_type=F32).astype(BF16)
        put[...] = jnp.concatenate([hot, hot, hot], axis=1)

    hot_of(rows_ref[...], row_blocks, row_pick, row_put)
    hot_of(cols_ref[...], col_blocks, col_pick, col_put)

    row_id = lax.broadcasted_iota(I32, (rows_p, LANE), 0)
    lane_id = lax.broadcasted_iota(I32, (rows_p, LANE), 1)
    lane_row = lax.broadcasted_iota(I32, (1, LANE), 1)
    eye = row_id == lane_id

    def to_row(column):
        return jnp.sum(jnp.where(eye, column, 0.0), axis=0, keepdims=True)

    def add_up(buf, n):
        parts = [buf[i] for i in range(n)]
        while len(parts) > 1:
            parts = [parts[i] + parts[i + 1] if i + 1 < len(parts) else parts[i]
                     for i in range(0, len(parts), 2)]
        return parts[0]

    def sum_all_devices(row, index):
        if direct:
            me = row_me * col_n + col_me
            buf = sum_all.at[index]
            buf[pl.ds(me, 1), :] = row
            pairs = [(a, b) for a in range(row_n) for b in range(col_n) if a or b]
            pairs.sort(key=lambda p: -(p[0] // 2 + bin(p[1]).count("1")))
            copies = []
            for k, (a, b) in enumerate(pairs):
                where = {"row": partner(row_me, a, row_n), "col": partner(col_me, b, col_n)}
                copy = pltpu.make_async_remote_copy(
                    src_ref=buf.at[pl.ds(me, 1)], dst_ref=buf.at[pl.ds(me, 1)], send_sem=send_sem.at[k],
                    recv_sem=sum_all_sem.at[index, k], device_id=where,
                    device_id_type=pl.DeviceIdType.MESH)
                copy.start()
                copies.append(copy)
            finish(copies)
            return jnp.sum(buf[...], axis=0, keepdims=True)
        buf = sum_col.at[index]
        buf[pl.ds(col_me, 1), :] = row
        finish(send("col", col_me, col_n, lambda p: buf.at[pl.ds(col_me, 1)], lambda k: buf.at[pl.ds(col_me, 1)],
                    lambda k: send_sem.at[k], lambda k: sum_col_sem.at[index, k]))
        row = jnp.sum(buf[...], axis=0, keepdims=True)
        buf = sum_row.at[index]
        buf[pl.ds(row_me, 1), :] = row
        finish(send("row", row_me, row_n, lambda p: buf.at[pl.ds(row_me, 1)], lambda k: buf.at[pl.ds(row_me, 1)],
                    lambda k: send_sem.at[k], lambda k: sum_row_sem.at[index, k]))
        return jnp.sum(buf[...], axis=0, keepdims=True)

    def coef(basis, place):
        acc = jnp.zeros((rows_p, LANE), F32)
        for j in range(basis.shape[1] // LANE):
            at = slice(j * LANE, (j + 1) * LANE)
            acc = acc + basis[:, at] * basis[place:place + 1, at]
        return to_row(jnp.sum(acc, axis=1, keepdims=True))

    def tables(gram, place):
        small = lax.dot_general(gram, gram, (((1,), (1,)), ((), ())), precision=HIGH, preferred_element_type=F32)
        square = jnp.concatenate([small, jnp.zeros((rows_p, LANE - rows_p), F32)], axis=1)
        one = jnp.where(eye & (row_id < place), 1.0, 0.0)
        return 2.0 * one - gram, one - (2.0 * gram - square), one

    def orth(basis, vec, row, place, table):
        both, left, one = table
        got = jnp.where(lane_row < place, row, 0.0)
        square = jnp.sum(jnp.where(lane_row == place, row, 0.0), axis=1, keepdims=True)
        column = jnp.sum(both * got, axis=1, keepdims=True)
        after = jnp.sum(left * got, axis=1, keepdims=True)
        first = jnp.sum(one * got, axis=1, keepdims=True)
        square = square - jnp.sum(column * (first + after), axis=0, keepdims=True)
        scale = jnp.sqrt(square + 1e-06)
        inverse = 1.0 / scale
        spread = jnp.broadcast_to(jnp.where(row_id[:, 0:1] == place, 1.0, -column), (rows_p, LANE))
        for j in range(basis.shape[1] // LANE):
            at = slice(j * LANE, (j + 1) * LANE)
            s, h = j * LANE // tile, j * LANE % tile
            vec[s:s + 1, h:h + LANE] = jnp.sum(spread * basis[:, at], axis=0, keepdims=True)
        out = vec[...] * inverse

        def grow(gram):
            for s in range(vec.shape[0]):
                basis[place:place + 1, s * tile:(s + 1) * tile] = out[s:s + 1, :]
            if gram is None:
                return None
            cross = after * inverse
            grown = jnp.where(row_id == place, to_row(cross), gram)
            grown = jnp.where(lane_id == place, cross, grown)
            corner = (row_id == place) & (lane_id == place)
            return jnp.where(corner, square / (scale * scale), grown)

        return scale, out, grow

    def matvec(gathered, n, pick, put, contract):
        full = jnp.concatenate([gathered[i].astype(F32) for i in range(n)], axis=0).astype(BF16)
        picked[...] = jnp.dot(pick[...], full, preferred_element_type=F32)
        sub = lax.broadcasted_iota(I32, (8, tile), 0)
        for g in range(slots // 8):
            left = picked[g * 8:(g + 1) * 8, :].astype(BF16)
            acc = jnp.zeros((8, tile), F32)
            for i in range(8):
                res = lax.dot_general(left, tiles[g * 8 + i], (((1,), (contract,)), ((), ())),
                                      preferred_element_type=F32)
                acc = jnp.where(sub == i, res, acc)
            products[g * 8:(g + 1) * 8, :] = acc
        full = products[...]
        high = full.astype(BF16)
        rest = full - high.astype(F32)
        middle = rest.astype(BF16)
        low = (rest - middle.astype(F32)).astype(BF16)
        return jnp.dot(put[...], jnp.concatenate([high, middle, low], axis=0), preferred_element_type=F32)

    def gather(axis, me, n, own, buf, sems, between):
        buf[me] = own.astype(BF16)
        copies = send(axis, me, n, lambda p: buf.at[me], lambda k: buf.at[me], lambda k: send_sem.at[k], sems)
        between()
        finish(copies)

    def scatter(axis, me, n, value, basis, place, sub, parts, recv, sems):
        for i in range(n):
            parts[i] = value[i * sub:(i + 1) * sub, :]
        finish(send(axis, me, n, lambda p: parts.at[p], lambda k: recv.at[k], lambda k: send_sem.at[k], sems))
        total = parts[me]
        for k in range(1, n):
            total = total + recv[k]
        for s in range(sub):
            basis[place:place + 1, s * tile:(s + 1) * tile] = total[s:s + 1, :]

    def kept(keep, source, target):
        factor = keep[...]
        high = factor.astype(BF16)
        low = (factor - high.astype(F32)).astype(BF16)
        left = jnp.concatenate(
            [jnp.concatenate([high, high], axis=1), jnp.concatenate([low, jnp.zeros(low.shape, BF16)], axis=1)], axis=0)
        step = min(512, target.shape[1])
        for j in range(target.shape[1] // step):
            at = slice(j * step, (j + 1) * step)
            data = jnp.concatenate([decode(source[i, :, at]) for i in range(source.shape[0])], axis=0)
            top = data.astype(BF16)
            rest = (data - top.astype(F32)).astype(BF16)
            both = jnp.dot(left, jnp.concatenate([top, rest], axis=0), preferred_element_type=F32)
            target[0:keep_p, at] = both[0:keep_p] + both[keep_p:2 * keep_p]

    def half_gram(basis):
        wide = basis[...]
        small = lax.dot_general(wide, wide, (((1,), (1,)), ((), ())), precision=HIGH, preferred_element_type=F32)
        full = jnp.concatenate([small, jnp.zeros((rows_p, LANE - rows_p), F32)], axis=1)
        packed = full[0:part]
        for g in range(1, fold):
            packed = packed + pltpu.roll(full[g * part:(g + 1) * part], g * width, 1)
        return packed

    def unpack(packed):
        pieces = [packed] + [pltpu.roll(packed, LANE - g * width, 1) for g in range(1, fold)]
        return jnp.where(lane_id < width, jnp.concatenate(pieces, axis=0), 0.0)

    def row_spread(buf, value, index):
        buf[row_me] = value
        return send("row", row_me, row_n, lambda p: buf.at[row_me], lambda k: buf.at[row_me],
                    lambda k: gram_send.at[index, k], lambda k: gram_recv.at[index, k])

    def col_spread(buf, value, index):
        buf[col_me] = value
        return send("col", col_me, col_n, lambda p: buf.at[col_me], lambda k: buf.at[col_me],
                    lambda k: gram_send.at[index, k], lambda k: gram_recv.at[index, k])

    own_next.wait()
    own_keep_v.wait()
    own_keep_u.wait()
    v_rows[keep_n:keep_n + 1, :] = v_first[...]
    finish(v_init)
    kept(keep_v, v_all, v_rows)
    v_copies = row_spread(gram_v_row, half_gram(v_rows), 0)
    finish(u_init)
    kept(keep_u, u_all, u_rows)
    u_copies = col_spread(gram_u_col, half_gram(u_rows), 1)
    finish(v_copies)
    v_copies = col_spread(gram_v_col, add_up(gram_v_row, row_n), 2)
    finish(u_copies)
    u_copies = row_spread(gram_u_row, add_up(gram_u_col, col_n), 3)
    finish(v_copies)
    wide = unpack(add_up(gram_v_col, col_n)) / v_total
    first_row = wide[keep_n:keep_n + 1, :]
    gram_v = jnp.where((row_id < keep_n) & (lane_id < keep_n), wide, 0.0)
    scale, out, grow = orth(v_rows, v_vec, first_row, keep_n, tables(gram_v, keep_n))

    state = {"v": gram_v, "u": None}

    def between_v(place, grow, step):
        def run():
            state["v"] = grow(state["v"])
            state["v_table"] = tables(state["v"], place + 1)
            if step == 0:
                finish(u_copies)
                gram_u = unpack(add_up(gram_u_row, row_n)) / u_total
                state["u"] = jnp.where((row_id < keep_n) & (lane_id < keep_n), gram_u, 0.0)
                state["u_table"] = tables(state["u"], keep_n)
        return run

    def between_u(place, grow, step):
        def run():
            if step + 1 < STEPS:
                state["u"] = grow(state["u"])
                state["u_table"] = tables(state["u"], place + 1)
            else:
                grow(None)
        return run

    alphas, betas = [], []
    for step in range(STEPS):
        u_place, v_place = keep_n + step, keep_n + 1 + step
        gather("row", row_me, row_n, out, v_gather.at[step], lambda k: vg_sem.at[step, k],
               between_v(v_place - 1, grow, step))
        if step == 0:
            own_t.wait()
        partial = matvec(v_gather.at[step], row_n, col_pick, row_put, 1)
        scatter("col", col_me, col_n, partial, u_rows, u_place, u_sub, u_parts, u_recv.at[step],
                lambda k: ur_sem.at[step, k])
        row = sum_all_devices(coef(u_rows, u_place), 2 * step) / u_total
        alpha, out, grow = orth(u_rows, u_vec, row, u_place, state["u_table"])
        gather("col", col_me, col_n, out, u_gather.at[step], lambda k: ug_sem.at[step, k],
               between_u(u_place, grow, step))
        partial = matvec(u_gather.at[step], col_n, row_pick, col_put, 0)
        scatter("row", row_me, row_n, partial, v_rows, v_place, v_sub, v_parts, v_recv.at[step],
                lambda k: vr_sem.at[step, k])
        row = sum_all_devices(coef(v_rows, v_place), 2 * step + 1) / v_total
        beta, out, grow = orth(v_rows, v_vec, row, v_place, state["v_table"])
        alphas.append(alpha)
        betas.append(beta)
    grow(None)
    place_r = lax.broadcasted_iota(I32, (8, LANE), 0)
    place_l = lax.broadcasted_iota(I32, (8, LANE), 1)
    result = jnp.zeros((8, LANE), F32)
    for step in range(STEPS):
        result = jnp.where((place_r == 0) & (place_l == step), alphas[step], result)
        result = jnp.where((place_r == 1) & (place_l == step), betas[step], result)
    bi_out[...] = result
    u_out[...] = u_rows[0:u_out.shape[0], :]
    v_out[...] = v_rows[0:v_out.shape[0], :]


def per_device(
    u_start, v_start, keep_u, keep_v, v_next, tile_blocks, tile_rows, tile_cols, tile_count
):
    row_n = lax.axis_size("row")
    col_n = lax.axis_size("col")
    u_here, v_here = u_start.shape[0], v_start.shape[0]
    basis, keep_n = keep_u.shape
    u_len = u_start.shape[1] // col_n
    v_len = v_start.shape[1] // row_n
    slots, tile = tile_blocks.shape[0], tile_blocks.shape[1]
    fold = max(f for f in (1, 2, 3) if f * (keep_n + 1) <= LANE)
    rows_p = -(-(keep_n + 1 + STEPS) // (8 * fold)) * 8 * fold
    keep_p = -(-keep_n // 8) * 8
    assert rows_p <= LANE
    pad = ((0, keep_p - keep_n), (0, 0))
    sums = 2 * STEPS
    total_n = row_n * col_n
    direct_n = total_n if total_n <= DIRECT else 1
    staged = 1 if total_n <= DIRECT else sums
    part = rows_p // fold
    dma = pltpu.SemaphoreType.DMA
    vmem = pl.BlockSpec(memory_space=pltpu.VMEM)
    hbm = pl.BlockSpec(memory_space=pltpu.HBM)
    u_sub, v_sub = u_len // tile, v_len // tile
    row_blocks, col_blocks = col_n * u_sub, row_n * v_sub
    most = max(row_n, col_n)
    u_basis, v_basis, bidiagonal = pl.pallas_call(
        functools.partial(kernel, row_n, col_n, keep_n, fold),
        out_shape=(
            jax.ShapeDtypeStruct((keep_n + STEPS, u_len), F32),
            jax.ShapeDtypeStruct((keep_n + 1 + STEPS, v_len), F32),
            jax.ShapeDtypeStruct((8, LANE), F32),
        ),
        in_specs=[hbm] * 9,
        out_specs=(vmem, vmem, vmem),
        scratch_shapes=[
            pltpu.VMEM(u_start.shape, F32),
            pltpu.VMEM(v_start.shape, F32),
            pltpu.VMEM((col_n, u_here, u_len), I16),
            pltpu.VMEM((row_n, v_here, v_len), I16),
            pltpu.VMEM((col_n, u_here, u_len), I16),
            pltpu.VMEM((row_n, v_here, v_len), I16),
            pltpu.VMEM(tile_blocks.shape, BF16),
            pltpu.VMEM((keep_p, basis), F32),
            pltpu.VMEM((keep_p, basis), F32),
            pltpu.VMEM((1, v_len), F32),
            pltpu.VMEM((1, slots), I32),
            pltpu.VMEM((1, slots), I32),
            pltpu.VMEM((1, 1), I32),
            pltpu.VMEM((rows_p, u_len), F32),
            pltpu.VMEM((rows_p, v_len), F32),
            pltpu.VMEM((u_sub, tile), F32),
            pltpu.VMEM((v_sub, tile), F32),
            pltpu.VMEM((row_n, part, LANE), F32),
            pltpu.VMEM((col_n, part, LANE), F32),
            pltpu.VMEM((col_n, part, LANE), F32),
            pltpu.VMEM((row_n, part, LANE), F32),
            pltpu.VMEM((staged, col_n, LANE), F32),
            pltpu.VMEM((staged, row_n, LANE), F32),
            pltpu.VMEM((sums, direct_n, LANE), F32),
            pltpu.VMEM((STEPS, row_n, v_sub, tile), BF16),
            pltpu.VMEM((STEPS, col_n, u_sub, tile), BF16),
            pltpu.VMEM((col_n, u_sub, tile), F32),
            pltpu.VMEM((row_n, v_sub, tile), F32),
            pltpu.VMEM((STEPS, col_n, u_sub, tile), F32),
            pltpu.VMEM((STEPS, row_n, v_sub, tile), F32),
            pltpu.VMEM((slots, row_blocks), BF16),
            pltpu.VMEM((slots, col_blocks), BF16),
            pltpu.VMEM((row_blocks, 3 * slots), BF16),
            pltpu.VMEM((col_blocks, 3 * slots), BF16),
            pltpu.VMEM((slots, tile), F32),
            pltpu.VMEM((slots, tile), F32),
            dma((9,)),
            dma((col_n,)),
            dma((col_n,)),
            dma((row_n,)),
            dma((row_n,)),
            dma((max(most, direct_n),)),
            dma((4, most)),
            dma((4, most)),
            dma((staged, col_n)),
            dma((staged, row_n)),
            dma((sums, direct_n)),
            dma((STEPS, row_n)),
            dma((STEPS, col_n)),
            dma((STEPS, col_n)),
            dma((STEPS, row_n)),
        ],
        compiler_params=pltpu.CompilerParams(
            collective_id=0, has_side_effects=True, vmem_limit_bytes=62 * 1024 * 1024
        ),
    )(
        u_start, v_start, jnp.pad(keep_u.T, pad), jnp.pad(keep_v.T, pad), v_next.reshape(1, -1), tile_blocks,
        tile_rows.reshape(1, -1), tile_cols.reshape(1, -1), tile_count.reshape(1, 1),
    )
    return u_basis, v_basis, bidiagonal[:2, :STEPS]


def solution(mesh):
    return jax.shard_map(
        per_device,
        mesh=mesh,
        in_specs=(
            P("col", "row"),
            P("row", "col"),
            P(),
            P(),
            P(("col", "row")),
            P(("row", "col"), None, None),
            P(("row", "col")),
            P(("row", "col")),
            P(("row", "col")),
        ),
        out_specs=(P(None, ("row", "col")), P(None, ("col", "row")), P()),
        check_vma=False,
    )
```

```python
import functools

import jax
import jax.numpy as jnp
from jax import lax
from jax.experimental import pallas as pl
from jax.experimental.pallas import tpu as pltpu
from jax.sharding import PartitionSpec as P

STEPS = 2
HIGH = lax.Precision.HIGHEST
F32 = jnp.float32
BF16 = jnp.bfloat16
I16 = jnp.int16
I32 = jnp.int32
LANE = 128
DIRECT = 32
KNEE = 5.0
FINE = 4800.0
COARSE = 461.0


def encode(x):
    code = x * COARSE + jnp.clip(x, -KNEE, KNEE) * (FINE - COARSE)
    return jnp.round(code).astype(I32).astype(I16)


def decode(code):
    y = code.astype(I32).astype(F32)
    near = jnp.clip(y, -KNEE * FINE, KNEE * FINE)
    return near * (1.0 / FINE) + (y - near) * (1.0 / COARSE)


def partner(me, k, n):
    if n & (n - 1):
        return lax.rem(me + k, n)
    other, bit = 0, 1
    while bit < n:
        digit = lax.rem(lax.div(me, bit), 2)
        other = other + (1 - digit if k & bit else digit) * bit
        bit *= 2
    return other


def kernel(
    row_n, col_n, keep_n, u_hbm, v_hbm, keep_u_hbm, keep_v_hbm, v_next_hbm, tiles_hbm, rows_hbm, cols_hbm,
    count_hbm,
    u_out, v_out, bi_out,
    u_in, v_in, u_code, v_code, u_all, v_all, tiles, turned, unit, keep_u, keep_v, v_first, rows_ref, cols_ref, count_ref,
    u_rows, v_rows, u_vec, v_vec, gram_v_col, gram_v_row, gram_u_col, gram_u_row,
    sum_col, sum_row, sum_all, v_gather, u_gather, u_parts, v_parts, u_recv, v_recv,
    row_pick, col_pick, row_put, col_put, picked, products,
    local_sem, init_u_send, init_u_recv, init_v_send, init_v_recv, send_sem, gram_send, gram_recv,
    sum_col_sem, sum_row_sem, sum_all_sem, vg_sem, ug_sem, ur_sem, vr_sem,
):
    row_me = lax.axis_index("row")
    col_me = lax.axis_index("col")

    def load(index, source, target):
        copy = pltpu.make_async_copy(source, target, local_sem.at[index])
        copy.start()
        return copy

    own_v = load(0, v_hbm, v_in)
    own_keep_v = load(2, keep_v_hbm, keep_v)
    own_keep_u = load(3, keep_u_hbm, keep_u)
    own_next = load(4, v_next_hbm, v_first)
    own_places = [load(5, rows_hbm, rows_ref), load(6, cols_hbm, cols_ref), load(7, count_hbm, count_ref)]
    own_u = load(1, u_hbm, u_in)

    barrier = pltpu.get_barrier_semaphore()
    for k in range(1, row_n):
        pl.semaphore_signal(barrier, inc=1, device_id={"row": partner(row_me, k, row_n)},
                            device_id_type=pl.DeviceIdType.MESH)
    for k in range(1, col_n):
        pl.semaphore_signal(barrier, inc=1, device_id={"col": partner(col_me, k, col_n)},
                            device_id_type=pl.DeviceIdType.MESH)

    direct = row_n * col_n <= DIRECT
    v_here, u_here = v_all.shape[1], u_all.shape[1]
    u_len, v_len = u_rows.shape[1], v_rows.shape[1]
    u_total = float(u_len * row_n * col_n)
    v_total = float(v_len * row_n * col_n)
    rows_p = u_rows.shape[0]
    keep_p = keep_u.shape[0]
    tile = tiles.shape[1]
    slots = tiles.shape[0]
    u_sub, v_sub = u_len // tile, v_len // tile
    row_blocks, col_blocks = col_n * u_sub, row_n * v_sub
    real = keep_n + 1
    starts, places = [], 0
    for g in range(-(-real // 8)):
        starts.append((8 * g, places - 8 * g))
        places += real - 8 * g
    assert places <= LANE

    def send(axis, me, n, src, dst, sends, recvs):
        copies = []
        for k in range(n - 1, 0, -1):
            target = partner(me, k, n)
            copy = pltpu.make_async_remote_copy(
                src_ref=src(target), dst_ref=dst(k), send_sem=sends(k), recv_sem=recvs(k),
                device_id={axis: target}, device_id_type=pl.DeviceIdType.MESH)
            copy.start()
            copies.append(copy)
        return copies

    def finish(copies):
        for copy in copies:
            copy.wait()

    sent = []

    def flight(copies, between=lambda: None):
        for copy in sent:
            copy.wait_send()
        sent[:] = copies
        between()
        for copy in copies:
            copy.wait_recv()

    phases = [0]

    def send_sems():
        turn = phases[0] % 2
        phases[0] += 1
        return lambda k: send_sem.at[turn, k]

    blank = keep_n // 8 * 8
    u_rows[blank:rows_p, :] = jnp.zeros((rows_p - blank, u_len), F32)
    v_rows[blank:rows_p, :] = jnp.zeros((rows_p - blank, v_len), F32)
    own_v.wait()
    for p in range(row_n):
        v_code[p] = encode(v_in[:, p * v_len:(p + 1) * v_len])
    pl.semaphore_wait(barrier, row_n + col_n - 2)
    v_init = send("row", row_me, row_n, lambda p: v_code.at[p], lambda k: v_all.at[row_me],
                  lambda k: init_v_send.at[k], lambda k: init_v_recv.at[k])
    own_u.wait()
    own_t = load(8, tiles_hbm, tiles)
    for p in range(col_n):
        u_code[p] = encode(u_in[:, p * u_len:(p + 1) * u_len])
    u_init = send("col", col_me, col_n, lambda p: u_code.at[p], lambda k: u_all.at[col_me],
                  lambda k: init_u_send.at[k], lambda k: init_u_recv.at[k])
    v_all[row_me] = v_code[row_me]
    u_all[col_me] = u_code[col_me]

    for copy in own_places:
        copy.wait()
    active = lax.broadcasted_iota(I32, (1, slots), 1) < count_ref[...]

    def hot_of(places, blocks, pick, put):
        hot = jnp.where(
            (lax.broadcasted_iota(I32, (blocks, slots), 0) == places) & active, 1.0, 0.0).astype(BF16)
        eye = (lax.broadcasted_iota(I32, (blocks, blocks), 0)
               == lax.broadcasted_iota(I32, (blocks, blocks), 1))
        pick[...] = lax.dot_general(hot, jnp.where(eye, 1.0, 0.0).astype(BF16), (((0,), (0,)), ((), ())),
                                    preferred_element_type=F32).astype(BF16)
        put[...] = jnp.concatenate([hot, hot, hot], axis=1)

    hot_of(rows_ref[...], row_blocks, row_pick, row_put)
    hot_of(cols_ref[...], col_blocks, col_pick, col_put)

    own_t.wait()
    unit[...] = jnp.where(lax.broadcasted_iota(I32, (tile, tile), 0) == lax.broadcasted_iota(I32, (tile, tile), 1),
                          1.0, 0.0).astype(BF16)

    def turn(g, carry):
        base = pl.multiple_of(g * 8, 8)
        for i in range(8):
            turned[base + i] = lax.dot_general(unit[...], tiles[base + i], (((1,), (1,)), ((), ())),
                                               preferred_element_type=F32).astype(BF16)
        return carry

    lax.fori_loop(0, slots // 8, turn, 0)

    row_id = lax.broadcasted_iota(I32, (rows_p, LANE), 0)
    lane_id = lax.broadcasted_iota(I32, (rows_p, LANE), 1)
    lane_row = lax.broadcasted_iota(I32, (1, LANE), 1)
    eye = row_id == lane_id

    def to_row(column):
        return jnp.sum(jnp.where(eye, column, 0.0), axis=0, keepdims=True)

    def add_up(buf, n):
        parts = [buf[i] for i in range(n)]
        while len(parts) > 1:
            parts = [parts[i] + parts[i + 1] if i + 1 < len(parts) else parts[i]
                     for i in range(0, len(parts), 2)]
        return parts[0]

    def sum_all_devices(row, index):
        if direct:
            me = row_me * col_n + col_me
            buf = sum_all.at[index]
            buf[pl.ds(me, 1), :] = row
            pairs = [(a, b) for a in range(row_n) for b in range(col_n) if a or b]
            pairs.sort(key=lambda p: -(p[0] // 2 + bin(p[1]).count("1")))
            copies, sends = [], send_sems()
            for k, (a, b) in enumerate(pairs):
                where = {"row": partner(row_me, a, row_n), "col": partner(col_me, b, col_n)}
                copy = pltpu.make_async_remote_copy(
                    src_ref=buf.at[pl.ds(me, 1)], dst_ref=buf.at[pl.ds(me, 1)], send_sem=sends(k),
                    recv_sem=sum_all_sem.at[index, k], device_id=where,
                    device_id_type=pl.DeviceIdType.MESH)
                copy.start()
                copies.append(copy)
            flight(copies)
            return jnp.sum(buf[...], axis=0, keepdims=True)
        buf = sum_col.at[index]
        buf[pl.ds(col_me, 1), :] = row
        flight(send("col", col_me, col_n, lambda p: buf.at[pl.ds(col_me, 1)], lambda k: buf.at[pl.ds(col_me, 1)],
                    send_sems(), lambda k: sum_col_sem.at[index, k]))
        row = jnp.sum(buf[...], axis=0, keepdims=True)
        buf = sum_row.at[index]
        buf[pl.ds(row_me, 1), :] = row
        flight(send("row", row_me, row_n, lambda p: buf.at[pl.ds(row_me, 1)], lambda k: buf.at[pl.ds(row_me, 1)],
                    send_sems(), lambda k: sum_row_sem.at[index, k]))
        return jnp.sum(buf[...], axis=0, keepdims=True)

    def coef(basis, place):
        acc = jnp.zeros((rows_p, LANE), F32)
        for j in range(basis.shape[1] // LANE):
            at = slice(j * LANE, (j + 1) * LANE)
            acc = acc + basis[:, at] * basis[place:place + 1, at]
        return to_row(jnp.sum(acc, axis=1, keepdims=True))

    def tables(gram, place):
        small = lax.dot_general(gram, gram, (((1,), (1,)), ((), ())), precision=HIGH, preferred_element_type=F32)
        square = jnp.concatenate([small, jnp.zeros((rows_p, LANE - rows_p), F32)], axis=1)
        one = jnp.where(eye & (row_id < place), 1.0, 0.0)
        return 2.0 * one - gram, one - (2.0 * gram - square), one

    def orth(basis, vec, row, place, table):
        both, left, one = table
        got = jnp.where(lane_row < place, row, 0.0)
        square = jnp.sum(jnp.where(lane_row == place, row, 0.0), axis=1, keepdims=True)
        column = jnp.sum(both * got, axis=1, keepdims=True)
        square = square - jnp.sum(column * jnp.sum((one + left) * got, axis=1, keepdims=True), axis=0, keepdims=True)
        scale = jnp.sqrt(square + 1e-06)
        inverse = 1.0 / scale
        spread = jnp.broadcast_to(jnp.where(row_id[:, 0:1] == place, 1.0, -column), (rows_p, LANE))
        for j in range(basis.shape[1] // LANE):
            at = slice(j * LANE, (j + 1) * LANE)
            s, h = j * LANE // tile, j * LANE % tile
            vec[s:s + 1, h:h + LANE] = jnp.sum(spread * basis[:, at], axis=0, keepdims=True)
        out = vec[...] * inverse

        def grow(gram):
            for s in range(vec.shape[0]):
                basis[place:place + 1, s * tile:(s + 1) * tile] = out[s:s + 1, :]
            if gram is None:
                return None
            cross = jnp.sum(left * got, axis=1, keepdims=True) * inverse
            grown = jnp.where(row_id == place, to_row(cross), gram)
            grown = jnp.where(lane_id == place, cross, grown)
            corner = (row_id == place) & (lane_id == place)
            return jnp.where(corner, square / (scale * scale), grown)

        return scale, out, grow

    def matvec(gathered, n, pick, put, blocks):
        full = jnp.concatenate([gathered[i].astype(F32) for i in range(n)], axis=0).astype(BF16)
        picked[...] = jnp.dot(pick[...], full, preferred_element_type=F32)
        sub = lax.broadcasted_iota(I32, (8, tile), 0)
        for g in range(slots // 8):
            left = picked[g * 8:(g + 1) * 8, :].astype(BF16)
            acc = jnp.zeros((8, tile), F32)
            for i in range(8):
                res = jnp.dot(left, blocks[g * 8 + i], preferred_element_type=F32)
                acc = jnp.where(sub == i, res, acc)
            products[g * 8:(g + 1) * 8, :] = acc
        full = products[...]
        high = full.astype(BF16)
        rest = full - high.astype(F32)
        middle = rest.astype(BF16)
        low = (rest - middle.astype(F32)).astype(BF16)
        return jnp.dot(put[...], jnp.concatenate([high, middle, low], axis=0), preferred_element_type=F32)

    def gather(axis, me, n, own, buf, sems, between):
        buf[me] = own.astype(BF16)
        flight(send(axis, me, n, lambda p: buf.at[me], lambda k: buf.at[me], send_sems(), sems), between)

    def scatter(axis, me, n, value, basis, place, sub, parts, recv, sems, between=lambda: None):
        for i in range(n):
            parts[i] = value[i * sub:(i + 1) * sub, :]
        flight(send(axis, me, n, lambda p: parts.at[p], lambda k: recv.at[k], send_sems(), sems), between)
        total = parts[me]
        for k in range(1, n):
            total = total + recv[k]
        for s in range(sub):
            basis[place:place + 1, s * tile:(s + 1) * tile] = total[s:s + 1, :]

    def kept(keep, source, target):
        factor = keep[...]
        high = factor.astype(BF16)
        low = (factor - high.astype(F32)).astype(BF16)
        left = jnp.concatenate(
            [jnp.concatenate([high, high], axis=1), jnp.concatenate([low, jnp.zeros(low.shape, BF16)], axis=1)], axis=0)
        step = min(512, target.shape[1])
        for j in range(target.shape[1] // step):
            at = slice(j * step, (j + 1) * step)
            data = jnp.concatenate([decode(source[i, :, at]) for i in range(source.shape[0])], axis=0)
            top = data.astype(BF16)
            rest = (data - top.astype(F32)).astype(BF16)
            both = jnp.dot(left, jnp.concatenate([top, rest], axis=0), preferred_element_type=F32)
            target[0:keep_p, at] = both[0:keep_p] + both[keep_p:2 * keep_p]

    def half_gram(basis):
        wide = basis[...]
        small = lax.dot_general(wide, wide, (((1,), (1,)), ((), ())), precision=HIGH, preferred_element_type=F32)
        full = jnp.concatenate([small, jnp.zeros((rows_p, LANE - rows_p), F32)], axis=1)
        packed = jnp.zeros((8, LANE), F32)
        for at, shift in starts:
            block = jnp.where((lane_id[0:8] >= at) & (lane_id[0:8] < real), full[at:at + 8], 0.0)
            packed = packed + (pltpu.roll(block, shift, 1) if shift else block)
        return packed

    def unpack(packed):
        pieces = []
        for at, shift in starts:
            block = pltpu.roll(packed, LANE - shift, 1) if shift else packed
            pieces.append(jnp.where((lane_id[0:8] >= at) & (lane_id[0:8] < real), block, 0.0))
        pieces.append(jnp.zeros((LANE - 8 * len(pieces), LANE), F32))
        upper = jnp.concatenate(pieces, axis=0)
        row_block = lax.div(lax.broadcasted_iota(I32, (LANE, LANE), 0), 8)
        lane_block = lax.div(lax.broadcasted_iota(I32, (LANE, LANE), 1), 8)
        full = upper + jnp.transpose(jnp.where(lane_block > row_block, upper, 0.0))
        return full[0:rows_p]

    def row_spread(buf, value, index):
        buf[row_me] = value
        return send("row", row_me, row_n, lambda p: buf.at[row_me], lambda k: buf.at[row_me],
                    lambda k: gram_send.at[index, k], lambda k: gram_recv.at[index, k])

    def col_spread(buf, value, index):
        buf[col_me] = value
        return send("col", col_me, col_n, lambda p: buf.at[col_me], lambda k: buf.at[col_me],
                    lambda k: gram_send.at[index, k], lambda k: gram_recv.at[index, k])

    early = []
    own_next.wait()
    own_keep_v.wait()
    own_keep_u.wait()
    v_rows[keep_n:keep_n + 1, :] = v_first[...]
    finish(v_init)
    kept(keep_v, v_all, v_rows)
    v_copies = col_spread(gram_v_col, half_gram(v_rows), 0)
    finish(v_copies)
    v_copies = row_spread(gram_v_row, add_up(gram_v_col, col_n), 1)
    finish(u_init)
    kept(keep_u, u_all, u_rows)
    u_copies = col_spread(gram_u_col, half_gram(u_rows), 2)
    finish(v_copies)
    wide = unpack(add_up(gram_v_row, row_n)) * (1.0 / v_total)
    first_row = wide[keep_n:keep_n + 1, :]
    gram_v = jnp.where((row_id < keep_n) & (lane_id < keep_n), wide, 0.0)
    scale, out, grow = orth(v_rows, v_vec, first_row, keep_n, tables(gram_v, keep_n))

    state = {"v": gram_v, "u": None}

    def write_kept():
        if blank:
            early.append(load(11, u_rows.at[0:blank], u_out.at[0:blank]))
            early.append(load(12, v_rows.at[0:blank], v_out.at[0:blank]))


    def between_v(place, grow, step):
        def run():
            state["v"] = grow(state["v"])
            state["v_table"] = tables(state["v"], place + 1)
            if step == 0:
                finish(u_copies)
                u_copies[:] = row_spread(gram_u_row, add_up(gram_u_col, col_n), 3)
        return run

    def gram_end():
        finish(u_copies)
        gram_u = unpack(add_up(gram_u_row, row_n)) * (1.0 / u_total)
        state["u"] = jnp.where((row_id < keep_n) & (lane_id < keep_n), gram_u, 0.0)
        state["u_table"] = tables(state["u"], keep_n)

    def between_u(place, grow, step):
        def run():
            if step + 1 < STEPS:
                state["u"] = grow(state["u"])
                state["u_table"] = tables(state["u"], place + 1)
            else:
                grow(None)
        return run

    alphas, betas = [], []
    for step in range(STEPS):
        u_place, v_place = keep_n + step, keep_n + 1 + step
        gather("row", row_me, row_n, out, v_gather.at[step], lambda k: vg_sem.at[step, k],
               between_v(v_place - 1, grow, step))
        partial = matvec(v_gather.at[step], row_n, col_pick, row_put, turned)
        scatter("col", col_me, col_n, partial, u_rows, u_place, u_sub, u_parts, u_recv.at[step],
                lambda k: ur_sem.at[step, k], gram_end if step == 0 else write_kept if step == 1 else lambda: None)
        row = sum_all_devices(coef(u_rows, u_place), 2 * step) * (1.0 / u_total)
        alpha, out, grow = orth(u_rows, u_vec, row, u_place, state["u_table"])
        gather("col", col_me, col_n, out, u_gather.at[step], lambda k: ug_sem.at[step, k],
               between_u(u_place, grow, step))
        partial = matvec(u_gather.at[step], col_n, row_pick, col_put, tiles)
        scatter("row", row_me, row_n, partial, v_rows, v_place, v_sub, v_parts, v_recv.at[step],
                lambda k: vr_sem.at[step, k])
        row = sum_all_devices(coef(v_rows, v_place), 2 * step + 1) * (1.0 / v_total)
        beta, out, grow = orth(v_rows, v_vec, row, v_place, state["v_table"])
        alphas.append(alpha)
        betas.append(beta)
    grow(None)
    place_r = lax.broadcasted_iota(I32, (8, LANE), 0)
    place_l = lax.broadcasted_iota(I32, (8, LANE), 1)
    result = jnp.zeros((8, LANE), F32)
    for step in range(STEPS):
        result = jnp.where((place_r == 0) & (place_l == step), alphas[step], result)
        result = jnp.where((place_r == 1) & (place_l == step), betas[step], result)
    bi_out[...] = result
    copies = [load(9, u_rows.at[blank:rows_p], u_out.at[blank:rows_p]),
              load(10, v_rows.at[blank:rows_p], v_out.at[blank:rows_p])]
    for copy in sent:
        copy.wait_send()
    finish(early)
    finish(copies)


def close(u_ref, v_ref, bi_ref, u_out, v_out, bi_out, u_in, v_in, bi_in, u_fit, v_fit, bi_fit, sem):
    sources = ((u_ref, u_in), (v_ref, v_in), (bi_ref, bi_in))
    loads = [pltpu.make_async_copy(a, b, sem.at[i]) for i, (a, b) in enumerate(sources)]
    for copy in loads:
        copy.start()
    stores = []
    for i, (copy, (here, fit, there)) in enumerate(zip(
            loads, ((u_in, u_fit, u_out), (v_in, v_fit, v_out), (bi_in, bi_fit, bi_out)))):
        copy.wait()
        fit[...] = here[0:fit.shape[0], 0:fit.shape[1]]
        store = pltpu.make_async_copy(fit, there, sem.at[3 + i])
        store.start()
        stores.append(store)
    for store in stores:
        store.wait()


def per_device(
    u_start, v_start, keep_u, keep_v, v_next, tile_blocks, tile_rows, tile_cols, tile_count
):
    row_n = lax.axis_size("row")
    col_n = lax.axis_size("col")
    u_here, v_here = u_start.shape[0], v_start.shape[0]
    basis, keep_n = keep_u.shape
    u_len = u_start.shape[1] // col_n
    v_len = v_start.shape[1] // row_n
    slots, tile = tile_blocks.shape[0], tile_blocks.shape[1]
    rows_p = -(-(keep_n + 1 + STEPS) // 8) * 8
    keep_p = -(-keep_n // 8) * 8
    assert rows_p <= LANE
    pad = ((0, keep_p - keep_n), (0, 0))
    sums = 2 * STEPS
    total_n = row_n * col_n
    direct_n = total_n if total_n <= DIRECT else 1
    staged = 1 if total_n <= DIRECT else sums
    dma = pltpu.SemaphoreType.DMA
    vmem = pl.BlockSpec(memory_space=pltpu.VMEM)
    hbm = pl.BlockSpec(memory_space=pltpu.HBM)
    u_sub, v_sub = u_len // tile, v_len // tile
    row_blocks, col_blocks = col_n * u_sub, row_n * v_sub
    most = max(row_n, col_n)
    padded = pl.pallas_call(
        functools.partial(kernel, row_n, col_n, keep_n),
        out_shape=(
            jax.ShapeDtypeStruct((rows_p, u_len), F32),
            jax.ShapeDtypeStruct((rows_p, v_len), F32),
            jax.ShapeDtypeStruct((8, LANE), F32),
        ),
        in_specs=[hbm] * 9,
        out_specs=(hbm, hbm, vmem),
        scratch_shapes=[
            pltpu.VMEM(u_start.shape, F32),
            pltpu.VMEM(v_start.shape, F32),
            pltpu.VMEM((col_n, u_here, u_len), I16),
            pltpu.VMEM((row_n, v_here, v_len), I16),
            pltpu.VMEM((col_n, u_here, u_len), I16),
            pltpu.VMEM((row_n, v_here, v_len), I16),
            pltpu.VMEM(tile_blocks.shape, BF16),
            pltpu.VMEM(tile_blocks.shape, BF16),
            pltpu.VMEM((tile, tile), BF16),
            pltpu.VMEM((keep_p, basis), F32),
            pltpu.VMEM((keep_p, basis), F32),
            pltpu.VMEM((1, v_len), F32),
            pltpu.VMEM((1, slots), I32),
            pltpu.VMEM((1, slots), I32),
            pltpu.VMEM((1, 1), I32),
            pltpu.VMEM((rows_p, u_len), F32),
            pltpu.VMEM((rows_p, v_len), F32),
            pltpu.VMEM((u_sub, tile), F32),
            pltpu.VMEM((v_sub, tile), F32),
            pltpu.VMEM((col_n, 8, LANE), F32),
            pltpu.VMEM((row_n, 8, LANE), F32),
            pltpu.VMEM((col_n, 8, LANE), F32),
            pltpu.VMEM((row_n, 8, LANE), F32),
            pltpu.VMEM((staged, col_n, LANE), F32),
            pltpu.VMEM((staged, row_n, LANE), F32),
            pltpu.VMEM((sums, direct_n, LANE), F32),
            pltpu.VMEM((STEPS, row_n, v_sub, tile), BF16),
            pltpu.VMEM((STEPS, col_n, u_sub, tile), BF16),
            pltpu.VMEM((col_n, u_sub, tile), F32),
            pltpu.VMEM((row_n, v_sub, tile), F32),
            pltpu.VMEM((STEPS, col_n, u_sub, tile), F32),
            pltpu.VMEM((STEPS, row_n, v_sub, tile), F32),
            pltpu.VMEM((slots, row_blocks), BF16),
            pltpu.VMEM((slots, col_blocks), BF16),
            pltpu.VMEM((row_blocks, 3 * slots), BF16),
            pltpu.VMEM((col_blocks, 3 * slots), BF16),
            pltpu.VMEM((slots, tile), F32),
            pltpu.VMEM((slots, tile), F32),
            dma((13,)),
            dma((col_n,)),
            dma((col_n,)),
            dma((row_n,)),
            dma((row_n,)),
            dma((2, max(most, direct_n))),
            dma((4, most)),
            dma((4, most)),
            dma((staged, col_n)),
            dma((staged, row_n)),
            dma((sums, direct_n)),
            dma((STEPS, row_n)),
            dma((STEPS, col_n)),
            dma((STEPS, col_n)),
            dma((STEPS, row_n)),
        ],
        compiler_params=pltpu.CompilerParams(
            collective_id=0, has_side_effects=True, vmem_limit_bytes=62 * 1024 * 1024
        ),
    )(
        u_start, v_start, jnp.pad(keep_u.T, pad), jnp.pad(keep_v.T, pad), v_next.reshape(1, -1), tile_blocks,
        tile_rows.reshape(1, -1), tile_cols.reshape(1, -1), tile_count.reshape(1, 1),
    )
    final = (
        jax.ShapeDtypeStruct((keep_n + STEPS, u_len), F32),
        jax.ShapeDtypeStruct((keep_n + 1 + STEPS, v_len), F32),
        jax.ShapeDtypeStruct((2, STEPS), F32),
    )
    return pl.pallas_call(
        close,
        out_shape=final,
        in_specs=[hbm] * 3,
        out_specs=(hbm, hbm, hbm),
        scratch_shapes=[pltpu.VMEM(x.shape, F32) for x in (*padded, *final)] + [dma((6,))],
        compiler_params=pltpu.CompilerParams(vmem_limit_bytes=62 * 1024 * 1024),
    )(*padded)


def solution(mesh):
    return jax.shard_map(
        per_device,
        mesh=mesh,
        in_specs=(
            P("col", "row"),
            P("row", "col"),
            P(),
            P(),
            P(("col", "row")),
            P(("row", "col"), None, None),
            P(("row", "col")),
            P(("row", "col")),
            P(("row", "col")),
        ),
        out_specs=(P(None, ("row", "col")), P(None, ("col", "row")), P()),
        check_vma=False,
    )
```

```python
import functools

import jax
import jax.numpy as jnp
from jax import lax
from jax.experimental import pallas as pl
from jax.experimental.pallas import tpu as pltpu
from jax.sharding import PartitionSpec as P

STEPS = 2
HIGH = lax.Precision.HIGHEST
F32 = jnp.float32
BF16 = jnp.bfloat16
I16 = jnp.int16
I32 = jnp.int32
LANE = 128
DIRECT = 32
KNEE = 5.0
FINE = 4800.0
COARSE = 461.0
LARGEST = 24.0


def encode(x, coarse=COARSE):
    code = x * coarse + jnp.clip(x, -KNEE, KNEE) * (FINE - coarse)
    return jnp.round(code).astype(I32).astype(I16)


def decode(code, coarse=COARSE):
    y = code.astype(I32).astype(F32)
    near = jnp.clip(y, -KNEE * FINE, KNEE * FINE)
    return near * (1.0 / FINE) + (y - near) * (1.0 / coarse)


def partner(me, k, n):
    if n & (n - 1):
        return lax.rem(me + k, n)
    other, bit = 0, 1
    while bit < n:
        digit = lax.rem(lax.div(me, bit), 2)
        other = other + (1 - digit if k & bit else digit) * bit
        bit *= 2
    return other


def kernel(
    row_n, col_n, keep_n, u_hbm, v_hbm, keep_u_hbm, keep_v_hbm, v_next_hbm, tiles_hbm, rows_hbm, cols_hbm,
    count_hbm,
    u_out, v_out, bi_out,
    u_in, v_in, u_code, v_code, u_all, v_all, tiles, turned, unit, keep_u, keep_v, v_first, rows_ref, cols_ref, count_ref,
    u_rows, v_rows, u_vec, v_vec, gram_v_col, gram_v_row, gram_u_col, gram_u_row,
    sum_col, sum_row, sum_all, v_gather, u_gather, u_parts, v_parts, u_recv, v_recv,
    row_pick, col_pick, row_put, col_put, picked, products, full_code, full_u, full_y, x_full, new_full,
    local_sem, init_u_send, init_u_recv, init_v_send, init_v_recv, send_sem, gram_send, gram_recv,
    sum_col_sem, sum_row_sem, sum_all_sem, vg_sem, ug_sem, ur_sem, vr_sem,
    full_send, full_recv, xf_send, xf_recv,
):
    row_me = lax.axis_index("row")
    col_me = lax.axis_index("col")

    def load(index, source, target):
        copy = pltpu.make_async_copy(source, target, local_sem.at[index])
        copy.start()
        return copy

    own_v = load(0, v_hbm, v_in)
    own_keep_v = load(2, keep_v_hbm, keep_v)
    own_keep_u = load(3, keep_u_hbm, keep_u)
    own_next = load(4, v_next_hbm, v_first)
    own_places = [load(5, rows_hbm, rows_ref), load(6, cols_hbm, cols_ref), load(7, count_hbm, count_ref)]
    own_u = load(1, u_hbm, u_in)

    barrier = pltpu.get_barrier_semaphore()
    for k in range(1, row_n):
        pl.semaphore_signal(barrier, inc=1, device_id={"row": partner(row_me, k, row_n)},
                            device_id_type=pl.DeviceIdType.MESH)
    for k in range(1, col_n):
        pl.semaphore_signal(barrier, inc=1, device_id={"col": partner(col_me, k, col_n)},
                            device_id_type=pl.DeviceIdType.MESH)

    direct = row_n * col_n <= DIRECT
    v_here, u_here = v_all.shape[1], u_all.shape[1]
    u_len, v_len = u_rows.shape[1], v_rows.shape[1]
    u_total = float(u_len * row_n * col_n)
    v_total = float(v_len * row_n * col_n)
    rows_p = u_rows.shape[0]
    keep_p = keep_u.shape[0]
    tile = tiles.shape[1]
    slots = tiles.shape[0]
    u_sub, v_sub = u_len // tile, v_len // tile
    row_blocks, col_blocks = col_n * u_sub, row_n * v_sub
    wide_coarse = (32700.0 - KNEE * FINE) / (LARGEST * keep_u.shape[1] ** 0.5 - KNEE)
    real = keep_n + 1
    starts, places = [], 0
    for g in range(-(-real // 8)):
        starts.append((8 * g, places - 8 * g))
        places += real - 8 * g
    assert places <= LANE

    def send(axis, me, n, src, dst, sends, recvs):
        copies = []
        for k in range(n - 1, 0, -1):
            target = partner(me, k, n)
            copy = pltpu.make_async_remote_copy(
                src_ref=src(target), dst_ref=dst(k), send_sem=sends(k), recv_sem=recvs(k),
                device_id={axis: target}, device_id_type=pl.DeviceIdType.MESH)
            copy.start()
            copies.append(copy)
        return copies

    def finish(copies):
        for copy in copies:
            copy.wait()

    sent = []

    def flight(copies, between=lambda: None):
        for copy in sent:
            copy.wait_send()
        sent[:] = copies
        between()
        for copy in copies:
            copy.wait_recv()

    phases = [0]

    def send_sems():
        turn = phases[0] % 2
        phases[0] += 1
        return lambda k: send_sem.at[turn, k]

    blank = keep_n // 8 * 8
    u_rows[blank:rows_p, :] = jnp.zeros((rows_p - blank, u_len), F32)
    v_rows[blank:rows_p, :] = jnp.zeros((rows_p - blank, v_len), F32)
    own_v.wait()
    for p in range(row_n):
        v_code[p] = encode(v_in[:, p * v_len:(p + 1) * v_len])
    pl.semaphore_wait(barrier, row_n + col_n - 2)
    v_init = send("row", row_me, row_n, lambda p: v_code.at[p], lambda k: v_all.at[row_me],
                  lambda k: init_v_send.at[k], lambda k: init_v_recv.at[k])
    own_u.wait()
    own_t = load(8, tiles_hbm, tiles)
    for p in range(col_n):
        u_code[p] = encode(u_in[:, p * u_len:(p + 1) * u_len])
    u_init = send("col", col_me, col_n, lambda p: u_code.at[p], lambda k: u_all.at[col_me],
                  lambda k: init_u_send.at[k], lambda k: init_u_recv.at[k])
    v_all[row_me] = v_code[row_me]
    u_all[col_me] = u_code[col_me]

    for copy in own_places:
        copy.wait()
    active = lax.broadcasted_iota(I32, (1, slots), 1) < count_ref[...]

    def hot_of(places, blocks, pick, put):
        hot = jnp.where(
            (lax.broadcasted_iota(I32, (blocks, slots), 0) == places) & active, 1.0, 0.0).astype(BF16)
        eye = (lax.broadcasted_iota(I32, (blocks, blocks), 0)
               == lax.broadcasted_iota(I32, (blocks, blocks), 1))
        pick[...] = lax.dot_general(hot, jnp.where(eye, 1.0, 0.0).astype(BF16), (((0,), (0,)), ((), ())),
                                    preferred_element_type=F32).astype(BF16)
        put[...] = jnp.concatenate([hot, hot, hot], axis=1)

    hot_of(rows_ref[...], row_blocks, row_pick, row_put)
    hot_of(cols_ref[...], col_blocks, col_pick, col_put)

    own_t.wait()
    unit[...] = jnp.where(lax.broadcasted_iota(I32, (tile, tile), 0) == lax.broadcasted_iota(I32, (tile, tile), 1),
                          1.0, 0.0).astype(BF16)

    def turn(g, carry):
        base = pl.multiple_of(g * 8, 8)
        for i in range(8):
            turned[base + i] = lax.dot_general(unit[...], tiles[base + i], (((1,), (1,)), ((), ())),
                                               preferred_element_type=F32).astype(BF16)
        return carry

    lax.fori_loop(0, slots // 8, turn, 0)

    row_id = lax.broadcasted_iota(I32, (rows_p, LANE), 0)
    lane_id = lax.broadcasted_iota(I32, (rows_p, LANE), 1)
    lane_row = lax.broadcasted_iota(I32, (1, LANE), 1)
    eye = row_id == lane_id

    def to_row(column):
        return jnp.sum(jnp.where(eye, column, 0.0), axis=0, keepdims=True)

    def add_up(buf, n):
        parts = [buf[i] for i in range(n)]
        while len(parts) > 1:
            parts = [parts[i] + parts[i + 1] if i + 1 < len(parts) else parts[i]
                     for i in range(0, len(parts), 2)]
        return parts[0]

    def sum_all_devices(row, index, between=lambda: None):
        if direct:
            me = row_me * col_n + col_me
            buf = sum_all.at[index]
            buf[pl.ds(me, 1), :] = row
            pairs = [(a, b) for a in range(row_n) for b in range(col_n) if a or b]
            pairs.sort(key=lambda p: -(p[0] // 2 + bin(p[1]).count("1")))
            copies, sends = [], send_sems()
            for k, (a, b) in enumerate(pairs):
                where = {"row": partner(row_me, a, row_n), "col": partner(col_me, b, col_n)}
                copy = pltpu.make_async_remote_copy(
                    src_ref=buf.at[pl.ds(me, 1)], dst_ref=buf.at[pl.ds(me, 1)], send_sem=sends(k),
                    recv_sem=sum_all_sem.at[index, k], device_id=where,
                    device_id_type=pl.DeviceIdType.MESH)
                copy.start()
                copies.append(copy)
            flight(copies, between)
            return jnp.sum(buf[...], axis=0, keepdims=True)
        buf = sum_col.at[index]
        buf[pl.ds(col_me, 1), :] = row
        flight(send("col", col_me, col_n, lambda p: buf.at[pl.ds(col_me, 1)], lambda k: buf.at[pl.ds(col_me, 1)],
                    send_sems(), lambda k: sum_col_sem.at[index, k]), between)
        row = jnp.sum(buf[...], axis=0, keepdims=True)
        buf = sum_row.at[index]
        buf[pl.ds(row_me, 1), :] = row
        flight(send("row", row_me, row_n, lambda p: buf.at[pl.ds(row_me, 1)], lambda k: buf.at[pl.ds(row_me, 1)],
                    send_sems(), lambda k: sum_row_sem.at[index, k]))
        return jnp.sum(buf[...], axis=0, keepdims=True)

    def coef(basis, place):
        acc = jnp.zeros((rows_p, LANE), F32)
        for j in range(basis.shape[1] // LANE):
            at = slice(j * LANE, (j + 1) * LANE)
            acc = acc + basis[:, at] * basis[place:place + 1, at]
        return to_row(jnp.sum(acc, axis=1, keepdims=True))

    def tables(gram, place):
        small = lax.dot_general(gram, gram, (((1,), (1,)), ((), ())), precision=HIGH, preferred_element_type=F32)
        square = jnp.concatenate([small, jnp.zeros((rows_p, LANE - rows_p), F32)], axis=1)
        one = jnp.where(eye & (row_id < place), 1.0, 0.0)
        return 2.0 * one - gram, one - (2.0 * gram - square), one

    def solve(row, place, table):
        both, left, one = table
        got = jnp.where(lane_row < place, row, 0.0)
        square = jnp.sum(jnp.where(lane_row == place, row, 0.0), axis=1, keepdims=True)
        column = jnp.sum(both * got, axis=1, keepdims=True)
        square = square - jnp.sum(column * jnp.sum((one + left) * got, axis=1, keepdims=True), axis=0, keepdims=True)
        scale = jnp.sqrt(square + 1e-06)
        return got, left, square, column, scale, 1.0 / scale

    def apply(basis, vec, place, found):
        column, inverse = found[3], found[5]
        spread = jnp.broadcast_to(jnp.where(row_id[:, 0:1] == place, 1.0, -column), (rows_p, LANE))
        for j in range(basis.shape[1] // LANE):
            at = slice(j * LANE, (j + 1) * LANE)
            s, h = j * LANE // tile, j * LANE % tile
            vec[s:s + 1, h:h + LANE] = jnp.sum(spread * basis[:, at], axis=0, keepdims=True)
        return vec[...] * inverse

    def grow_basis(basis, place, found, out, gram):
        got, left, square, column, scale, inverse = found
        for s in range(out.shape[0]):
            basis[place:place + 1, s * tile:(s + 1) * tile] = out[s:s + 1, :]
        if gram is None:
            return None
        cross = jnp.sum(left * got, axis=1, keepdims=True) * inverse
        grown = jnp.where(row_id == place, to_row(cross), gram)
        grown = jnp.where(lane_id == place, cross, grown)
        corner = (row_id == place) & (lane_id == place)
        return jnp.where(corner, square / (scale * scale), grown)

    def apply_full(step, found):
        column, inverse = found[3], found[5]
        spread = jnp.broadcast_to(jnp.where(row_id[0:keep_p, 0:1] < keep_n, -column[0:keep_p], 0.0), (keep_p, LANE))
        for q in range(col_n):
            for j in range(u_len // LANE):
                at = slice(j * LANE, (j + 1) * LANE)
                s, h = q * u_sub + j * LANE // tile, j * LANE % tile
                full_y[s:s + 1, h:h + LANE] = jnp.sum(spread * full_u[q, :, at], axis=0, keepdims=True)
        x = jnp.concatenate([x_full[step, q] for q in range(col_n)], axis=0)
        for old in range(step):
            before = jnp.concatenate([new_full[old, q] for q in range(col_n)], axis=0)
            x = x - column[keep_n + old:keep_n + old + 1, 0:1] * before
        return (x + full_y[...]) * inverse

    def joined(gathered, n):
        return jnp.concatenate([gathered[i].astype(F32) for i in range(n)], axis=0).astype(BF16)

    def matvec(full, pick, put, blocks):
        picked[...] = jnp.dot(pick[...], full, preferred_element_type=F32)
        sub = lax.broadcasted_iota(I32, (8, tile), 0)
        for g in range(slots // 8):
            left = picked[g * 8:(g + 1) * 8, :].astype(BF16)
            acc = jnp.zeros((8, tile), F32)
            for i in range(8):
                res = jnp.dot(left, blocks[g * 8 + i], preferred_element_type=F32)
                acc = jnp.where(sub == i, res, acc)
            products[g * 8:(g + 1) * 8, :] = acc
        full = products[...]
        high = full.astype(BF16)
        rest = full - high.astype(F32)
        middle = rest.astype(BF16)
        low = (rest - middle.astype(F32)).astype(BF16)
        return jnp.dot(put[...], jnp.concatenate([high, middle, low], axis=0), preferred_element_type=F32)

    def gather(axis, me, n, own, buf, sems, between):
        buf[me] = own.astype(BF16)
        flight(send(axis, me, n, lambda p: buf.at[me], lambda k: buf.at[me], send_sems(), sems), between)

    def scatter(axis, me, n, value, basis, place, sub, parts, recv, sems, between=lambda: None):
        for i in range(n):
            parts[i] = value[i * sub:(i + 1) * sub, :]
        flight(send(axis, me, n, lambda p: parts.at[p], lambda k: recv.at[k], send_sems(), sems), between)
        total = parts[me]
        for k in range(1, n):
            total = total + recv[k]
        for s in range(sub):
            basis[place:place + 1, s * tile:(s + 1) * tile] = total[s:s + 1, :]
        return total

    def kept(keep, source, target):
        factor = keep[...]
        high = factor.astype(BF16)
        low = (factor - high.astype(F32)).astype(BF16)
        left = jnp.concatenate(
            [jnp.concatenate([high, high], axis=1), jnp.concatenate([low, jnp.zeros(low.shape, BF16)], axis=1)], axis=0)
        step = min(512, target.shape[1])
        for j in range(target.shape[1] // step):
            at = slice(j * step, (j + 1) * step)
            data = jnp.concatenate([decode(source[i, :, at]) for i in range(source.shape[0])], axis=0)
            top = data.astype(BF16)
            rest = (data - top.astype(F32)).astype(BF16)
            both = jnp.dot(left, jnp.concatenate([top, rest], axis=0), preferred_element_type=F32)
            target[0:keep_p, at] = both[0:keep_p] + both[keep_p:2 * keep_p]

    def half_gram(basis):
        wide = basis[...]
        small = lax.dot_general(wide, wide, (((1,), (1,)), ((), ())), precision=HIGH, preferred_element_type=F32)
        full = jnp.concatenate([small, jnp.zeros((rows_p, LANE - rows_p), F32)], axis=1)
        packed = jnp.zeros((8, LANE), F32)
        for at, shift in starts:
            block = jnp.where((lane_id[0:8] >= at) & (lane_id[0:8] < real), full[at:at + 8], 0.0)
            packed = packed + (pltpu.roll(block, shift, 1) if shift else block)
        return packed

    def unpack(packed):
        pieces = []
        for at, shift in starts:
            block = pltpu.roll(packed, LANE - shift, 1) if shift else packed
            pieces.append(jnp.where((lane_id[0:8] >= at) & (lane_id[0:8] < real), block, 0.0))
        pieces.append(jnp.zeros((LANE - 8 * len(pieces), LANE), F32))
        upper = jnp.concatenate(pieces, axis=0)
        row_block = lax.div(lax.broadcasted_iota(I32, (LANE, LANE), 0), 8)
        lane_block = lax.div(lax.broadcasted_iota(I32, (LANE, LANE), 1), 8)
        full = upper + jnp.transpose(jnp.where(lane_block > row_block, upper, 0.0))
        return full[0:rows_p]

    def row_spread(buf, value, index):
        buf[row_me] = value
        return send("row", row_me, row_n, lambda p: buf.at[row_me], lambda k: buf.at[row_me],
                    lambda k: gram_send.at[index, k], lambda k: gram_recv.at[index, k])

    def col_spread(buf, value, index):
        buf[col_me] = value
        return send("col", col_me, col_n, lambda p: buf.at[col_me], lambda k: buf.at[col_me],
                    lambda k: gram_send.at[index, k], lambda k: gram_recv.at[index, k])

    early = []
    own_next.wait()
    own_keep_v.wait()
    own_keep_u.wait()
    v_rows[keep_n:keep_n + 1, :] = v_first[...]
    finish(v_init)
    kept(keep_v, v_all, v_rows)
    v_copies = col_spread(gram_v_col, half_gram(v_rows), 0)
    finish(u_init)
    kept(keep_u, u_all, u_rows)
    u_copies = col_spread(gram_u_col, half_gram(u_rows), 2)
    full_copies = []
    cut = u_len * 3 // 4

    def full_spread(index, a, b):
        full_copies.extend(send(
            "col", col_me, col_n, lambda p: full_code.at[col_me, :, a:b], lambda k: full_code.at[col_me, :, a:b],
            lambda k: full_send.at[index, k], lambda k: full_recv.at[index, k]))

    full_code[col_me] = encode(u_rows[0:keep_p, :], wide_coarse)
    full_spread(0, 0, cut)
    finish(v_copies)
    v_copies = row_spread(gram_v_row, add_up(gram_v_col, col_n), 1)
    finish(u_copies)
    u_copies = row_spread(gram_u_row, add_up(gram_u_col, col_n), 3)
    finish(v_copies)
    wide = unpack(add_up(gram_v_row, row_n)) * (1.0 / v_total)
    first_row = wide[keep_n:keep_n + 1, :]
    gram_v = jnp.where((row_id < keep_n) & (lane_id < keep_n), wide, 0.0)
    found = solve(first_row, keep_n, tables(gram_v, keep_n))
    out = apply(v_rows, v_vec, keep_n, found)

    state = {"v": gram_v, "u": None}

    def write_kept():
        if blank:
            early.append(load(11, u_rows.at[0:blank], u_out.at[0:blank]))
            early.append(load(12, v_rows.at[0:blank], v_out.at[0:blank]))


    def between_v(place, found, out, step):
        def run():
            state["v"] = grow_basis(v_rows, place, found, out, state["v"])
            state["v_table"] = tables(state["v"], place + 1)
            if step == 1:
                finish(full_copies)
                for q in range(col_n):
                    full_u[q] = decode(full_code[q], wide_coarse)
                full_u[col_me] = u_rows[0:keep_p, :]
        return run

    def grow_u(place, found, out, step):
        if step + 1 < STEPS:
            state["u"] = grow_basis(u_rows, place, found, out, state["u"])
            state["u_table"] = tables(state["u"], place + 1)
        else:
            grow_basis(u_rows, place, found, out, None)

    def gram_end():
        finish(u_copies)
        gram_u = unpack(add_up(gram_u_row, row_n)) * (1.0 / u_total)
        state["u"] = jnp.where((row_id < keep_n) & (lane_id < keep_n), gram_u, 0.0)
        state["u_table"] = tables(state["u"], keep_n)

    def between_u(place, grow, step):
        def run():
            if step + 1 < STEPS:
                state["u"] = grow(state["u"])
                state["u_table"] = tables(state["u"], place + 1)
            else:
                grow(None)
        return run

    def between_u(place, found, out, step):
        return lambda: grow_u(place, found, out, step)

    def share_new(out):
        def run():
            full_spread(1, cut, u_len)
            new_full[0, col_me] = out
            full_copies.extend(send(
                "col", col_me, col_n, lambda p: new_full.at[0, col_me], lambda k: new_full.at[0, col_me],
                lambda k: xf_send.at[0, k], lambda k: xf_recv.at[0, k]))
        return run

    def late_u(place, found, step):
        return lambda: grow_u(place, found, apply(u_rows, u_vec, place, found), step)

    alphas, betas = [], []
    for step in range(STEPS):
        u_place, v_place = keep_n + step, keep_n + 1 + step
        gather("row", row_me, row_n, out, v_gather.at[step], lambda k: vg_sem.at[step, k],
               between_v(v_place - 1, found, out, step))
        partial = matvec(joined(v_gather.at[step], row_n), col_pick, row_put, turned)
        total = scatter("col", col_me, col_n, partial, u_rows, u_place, u_sub, u_parts, u_recv.at[step],
                        lambda k: ur_sem.at[step, k],
                        gram_end if step == 0 else write_kept if step == 1 else lambda: None)
        if step == 0:
            row = sum_all_devices(coef(u_rows, u_place), 2 * step) * (1.0 / u_total)
            found = solve(row, u_place, state["u_table"])
            out = apply(u_rows, u_vec, u_place, found)
            gather("col", col_me, col_n, out, u_gather.at[step], lambda k: ug_sem.at[step, k],
                   between_u(u_place, found, out, step))
            full, between = joined(u_gather.at[step], col_n), share_new(out) if STEPS > 1 else lambda: None
        else:
            x_copies = []

            def share_x(step=step, total=total):
                x_full[step, col_me] = total
                x_copies.extend(send(
                    "col", col_me, col_n, lambda p: x_full.at[step, col_me], lambda k: x_full.at[step, col_me],
                    lambda k: xf_send.at[step, k], lambda k: xf_recv.at[step, k]))

            row = sum_all_devices(coef(u_rows, u_place), 2 * step, share_x) * (1.0 / u_total)
            found = solve(row, u_place, state["u_table"])
            finish(x_copies)
            wide = apply_full(step, found)
            if step + 1 < STEPS:
                for q in range(col_n):
                    new_full[step, q] = wide[q * u_sub:(q + 1) * u_sub]
            full, between = wide.astype(BF16), late_u(u_place, found, step)
        alphas.append(found[4])
        partial = matvec(full, row_pick, col_put, tiles)
        scatter("row", row_me, row_n, partial, v_rows, v_place, v_sub, v_parts, v_recv.at[step],
                lambda k: vr_sem.at[step, k], between)
        row = sum_all_devices(coef(v_rows, v_place), 2 * step + 1) * (1.0 / v_total)
        found = solve(row, v_place, state["v_table"])
        out = apply(v_rows, v_vec, v_place, found)
        betas.append(found[4])
    grow_basis(v_rows, keep_n + STEPS, found, out, None)
    place_r = lax.broadcasted_iota(I32, (8, LANE), 0)
    place_l = lax.broadcasted_iota(I32, (8, LANE), 1)
    result = jnp.zeros((8, LANE), F32)
    for step in range(STEPS):
        result = jnp.where((place_r == 0) & (place_l == step), alphas[step], result)
        result = jnp.where((place_r == 1) & (place_l == step), betas[step], result)
    bi_out[...] = result
    copies = [load(9, u_rows.at[blank:rows_p], u_out.at[blank:rows_p]),
              load(10, v_rows.at[blank:rows_p], v_out.at[blank:rows_p])]
    for copy in sent:
        copy.wait_send()
    finish(early)
    finish(copies)


def close(u_ref, v_ref, bi_ref, u_out, v_out, bi_out, u_in, v_in, bi_in, u_fit, v_fit, bi_fit, sem):
    pieces = [(bi_ref, bi_in, bi_fit, bi_out, None)]
    for here, inside, fit, there, n in ((u_ref, u_in, u_fit, u_out, 4), (v_ref, v_in, v_fit, v_out, 2)):
        step = here.shape[1] // n
        pieces += [(here, inside, fit, there, slice(i * step, (i + 1) * step)) for i in range(n)]
    loads = []
    for i, (here, inside, fit, there, at) in enumerate(pieces):
        source, target = (here, inside) if at is None else (here.at[:, at], inside.at[:, at])
        loads.append(pltpu.make_async_copy(source, target, sem.at[0, i]))
        loads[-1].start()
    stores = []
    for i, (here, inside, fit, there, at) in enumerate(pieces):
        loads[i].wait()
        if at is None:
            fit[...] = inside[0:fit.shape[0], 0:fit.shape[1]]
            store = pltpu.make_async_copy(fit, there, sem.at[1, i])
        else:
            fit[:, at] = inside[0:fit.shape[0], at]
            store = pltpu.make_async_copy(fit.at[:, at], there.at[:, at], sem.at[1, i])
        store.start()
        stores.append(store)
    for store in stores:
        store.wait()


def per_device(
    u_start, v_start, keep_u, keep_v, v_next, tile_blocks, tile_rows, tile_cols, tile_count
):
    row_n = lax.axis_size("row")
    col_n = lax.axis_size("col")
    u_here, v_here = u_start.shape[0], v_start.shape[0]
    basis, keep_n = keep_u.shape
    u_len = u_start.shape[1] // col_n
    v_len = v_start.shape[1] // row_n
    slots, tile = tile_blocks.shape[0], tile_blocks.shape[1]
    rows_p = -(-(keep_n + 1 + STEPS) // 8) * 8
    keep_p = -(-keep_n // 8) * 8
    assert rows_p <= LANE
    pad = ((0, keep_p - keep_n), (0, 0))
    sums = 2 * STEPS
    total_n = row_n * col_n
    direct_n = total_n if total_n <= DIRECT else 1
    staged = 1 if total_n <= DIRECT else sums
    dma = pltpu.SemaphoreType.DMA
    vmem = pl.BlockSpec(memory_space=pltpu.VMEM)
    hbm = pl.BlockSpec(memory_space=pltpu.HBM)
    u_sub, v_sub = u_len // tile, v_len // tile
    row_blocks, col_blocks = col_n * u_sub, row_n * v_sub
    most = max(row_n, col_n)
    padded = pl.pallas_call(
        functools.partial(kernel, row_n, col_n, keep_n),
        out_shape=(
            jax.ShapeDtypeStruct((rows_p, u_len), F32),
            jax.ShapeDtypeStruct((rows_p, v_len), F32),
            jax.ShapeDtypeStruct((8, LANE), F32),
        ),
        in_specs=[hbm] * 9,
        out_specs=(hbm, hbm, vmem),
        scratch_shapes=[
            pltpu.VMEM(u_start.shape, F32),
            pltpu.VMEM(v_start.shape, F32),
            pltpu.VMEM((col_n, u_here, u_len), I16),
            pltpu.VMEM((row_n, v_here, v_len), I16),
            pltpu.VMEM((col_n, u_here, u_len), I16),
            pltpu.VMEM((row_n, v_here, v_len), I16),
            pltpu.VMEM(tile_blocks.shape, BF16),
            pltpu.VMEM(tile_blocks.shape, BF16),
            pltpu.VMEM((tile, tile), BF16),
            pltpu.VMEM((keep_p, basis), F32),
            pltpu.VMEM((keep_p, basis), F32),
            pltpu.VMEM((1, v_len), F32),
            pltpu.VMEM((1, slots), I32),
            pltpu.VMEM((1, slots), I32),
            pltpu.VMEM((1, 1), I32),
            pltpu.VMEM((rows_p, u_len), F32),
            pltpu.VMEM((rows_p, v_len), F32),
            pltpu.VMEM((u_sub, tile), F32),
            pltpu.VMEM((v_sub, tile), F32),
            pltpu.VMEM((col_n, 8, LANE), F32),
            pltpu.VMEM((row_n, 8, LANE), F32),
            pltpu.VMEM((col_n, 8, LANE), F32),
            pltpu.VMEM((row_n, 8, LANE), F32),
            pltpu.VMEM((staged, col_n, LANE), F32),
            pltpu.VMEM((staged, row_n, LANE), F32),
            pltpu.VMEM((sums, direct_n, LANE), F32),
            pltpu.VMEM((STEPS, row_n, v_sub, tile), BF16),
            pltpu.VMEM((STEPS, col_n, u_sub, tile), BF16),
            pltpu.VMEM((col_n, u_sub, tile), F32),
            pltpu.VMEM((row_n, v_sub, tile), F32),
            pltpu.VMEM((STEPS, col_n, u_sub, tile), F32),
            pltpu.VMEM((STEPS, row_n, v_sub, tile), F32),
            pltpu.VMEM((slots, row_blocks), BF16),
            pltpu.VMEM((slots, col_blocks), BF16),
            pltpu.VMEM((row_blocks, 3 * slots), BF16),
            pltpu.VMEM((col_blocks, 3 * slots), BF16),
            pltpu.VMEM((slots, tile), F32),
            pltpu.VMEM((slots, tile), F32),
            pltpu.VMEM((col_n, keep_p, u_len), I16),
            pltpu.VMEM((col_n, keep_p, u_len), F32),
            pltpu.VMEM((row_blocks, tile), F32),
            pltpu.VMEM((STEPS, col_n, u_sub, tile), F32),
            pltpu.VMEM((STEPS, col_n, u_sub, tile), F32),
            dma((13,)),
            dma((col_n,)),
            dma((col_n,)),
            dma((row_n,)),
            dma((row_n,)),
            dma((2, max(most, direct_n))),
            dma((4, most)),
            dma((4, most)),
            dma((staged, col_n)),
            dma((staged, row_n)),
            dma((sums, direct_n)),
            dma((STEPS, row_n)),
            dma((STEPS, col_n)),
            dma((STEPS, col_n)),
            dma((STEPS, row_n)),
            dma((2, col_n)),
            dma((2, col_n)),
            dma((STEPS, col_n)),
            dma((STEPS, col_n)),
        ],
        compiler_params=pltpu.CompilerParams(
            collective_id=0, has_side_effects=True, vmem_limit_bytes=62 * 1024 * 1024
        ),
    )(
        u_start, v_start, jnp.pad(keep_u.T, pad), jnp.pad(keep_v.T, pad), v_next.reshape(1, -1), tile_blocks,
        tile_rows.reshape(1, -1), tile_cols.reshape(1, -1), tile_count.reshape(1, 1),
    )
    final = (
        jax.ShapeDtypeStruct((keep_n + STEPS, u_len), F32),
        jax.ShapeDtypeStruct((keep_n + 1 + STEPS, v_len), F32),
        jax.ShapeDtypeStruct((2, STEPS), F32),
    )
    return pl.pallas_call(
        close,
        out_shape=final,
        in_specs=[hbm] * 3,
        out_specs=(hbm, hbm, hbm),
        scratch_shapes=[pltpu.VMEM(x.shape, F32) for x in (*padded, *final)] + [dma((2, 7))],
        compiler_params=pltpu.CompilerParams(vmem_limit_bytes=62 * 1024 * 1024),
    )(*padded)


def solution(mesh):
    return jax.shard_map(
        per_device,
        mesh=mesh,
        in_specs=(
            P("col", "row"),
            P("row", "col"),
            P(),
            P(),
            P(("col", "row")),
            P(("row", "col"), None, None),
            P(("row", "col")),
            P(("row", "col")),
            P(("row", "col")),
        ),
        out_specs=(P(None, ("row", "col")), P(None, ("col", "row")), P()),
        check_vma=False,
    )
```

```python
import functools

import jax
import jax.numpy as jnp
from jax import lax
from jax.experimental import pallas as pl
from jax.experimental.pallas import tpu as pltpu
from jax.sharding import PartitionSpec as P

STEPS = 2
HIGH = lax.Precision.HIGHEST
F32 = jnp.float32
BF16 = jnp.bfloat16
I16 = jnp.int16
I32 = jnp.int32
LANE = 128
DIRECT = 32
KNEE = 5.0
FINE = 4800.0
COARSE = 461.0
LARGEST = 24.0


def encode(x, coarse=COARSE):
    code = x * coarse + jnp.clip(x, -KNEE, KNEE) * (FINE - coarse)
    return jnp.round(code).astype(I32).astype(I16)


def decode(code, coarse=COARSE):
    y = code.astype(I32).astype(F32)
    near = jnp.clip(y, -KNEE * FINE, KNEE * FINE)
    return near * (1.0 / FINE) + (y - near) * (1.0 / coarse)


def partner(me, k, n):
    if n & (n - 1):
        return lax.rem(me + k, n)
    other, bit = 0, 1
    while bit < n:
        digit = lax.rem(lax.div(me, bit), 2)
        other = other + (1 - digit if k & bit else digit) * bit
        bit *= 2
    return other


def kernel(
    row_n, col_n, keep_n, u_hbm, v_hbm, keep_u_hbm, keep_v_hbm, v_next_hbm, tiles_hbm, rows_hbm, cols_hbm,
    count_hbm,
    u_out, v_out, bi_out,
    u_in, v_in, u_code, v_code, u_all, v_all, tiles, turned, unit, keep_u, keep_v, v_first, rows_ref, cols_ref, count_ref,
    u_rows, v_rows, u_vec, v_vec, gram_v_col, gram_v_row, gram_u_col, gram_u_row,
    sum_col, sum_row, sum_all, v_gather, u_gather, u_parts, v_parts, u_recv, v_recv,
    row_pick, col_pick, row_put, col_put, picked, products, full_code, full_u, full_y, x_full, new_full,
    local_sem, init_u_send, init_u_recv, init_v_send, init_v_recv, send_sem, gram_send, gram_recv,
    sum_col_sem, sum_row_sem, sum_all_sem, vg_sem, ug_sem, ur_sem, vr_sem,
    full_send, full_recv, xf_send, xf_recv,
):
    row_me = lax.axis_index("row")
    col_me = lax.axis_index("col")

    def load(index, source, target):
        copy = pltpu.make_async_copy(source, target, local_sem.at[index])
        copy.start()
        return copy

    own_v = load(0, v_hbm, v_in)
    own_keep_v = load(2, keep_v_hbm, keep_v)
    own_keep_u = load(3, keep_u_hbm, keep_u)
    own_next = load(4, v_next_hbm, v_first)
    own_places = [load(5, rows_hbm, rows_ref), load(6, cols_hbm, cols_ref), load(7, count_hbm, count_ref)]
    own_u = load(1, u_hbm, u_in)

    barrier = pltpu.get_barrier_semaphore()
    for k in range(1, row_n):
        pl.semaphore_signal(barrier, inc=1, device_id={"row": partner(row_me, k, row_n)},
                            device_id_type=pl.DeviceIdType.MESH)
    for k in range(1, col_n):
        pl.semaphore_signal(barrier, inc=1, device_id={"col": partner(col_me, k, col_n)},
                            device_id_type=pl.DeviceIdType.MESH)

    direct = row_n * col_n <= DIRECT
    v_here, u_here = v_all.shape[1], u_all.shape[1]
    u_len, v_len = u_rows.shape[1], v_rows.shape[1]
    u_total = float(u_len * row_n * col_n)
    v_total = float(v_len * row_n * col_n)
    rows_p = u_rows.shape[0]
    keep_p = keep_u.shape[0]
    tile = tiles.shape[1]
    slots = tiles.shape[0]
    u_sub, v_sub = u_len // tile, v_len // tile
    row_blocks, col_blocks = col_n * u_sub, row_n * v_sub
    wide_coarse = (32700.0 - KNEE * FINE) / (LARGEST * keep_u.shape[1] ** 0.5 - KNEE)
    real = keep_n + 1
    starts, places = [], 0
    for g in range(-(-real // 8)):
        starts.append((8 * g, places - 8 * g))
        places += real - 8 * g
    assert places <= LANE

    def send(axis, me, n, src, dst, sends, recvs):
        copies = []
        for k in range(n - 1, 0, -1):
            target = partner(me, k, n)
            copy = pltpu.make_async_remote_copy(
                src_ref=src(target), dst_ref=dst(k), send_sem=sends(k), recv_sem=recvs(k),
                device_id={axis: target}, device_id_type=pl.DeviceIdType.MESH)
            copy.start()
            copies.append(copy)
        return copies

    def finish(copies):
        for copy in copies:
            copy.wait()

    sent = []

    def flight(copies, between=lambda: None, arrived=None):
        for copy in sent:
            copy.wait_send()
        sent[:] = copies
        between()
        if arrived is not None:
            arrived.wait()
            return
        for copy in copies:
            copy.wait_recv()

    phases = [0]

    def send_sems():
        turn = phases[0] % 2
        phases[0] += 1
        return lambda k: send_sem.at[turn, k]

    blank = keep_n // 8 * 8
    u_rows[blank:rows_p, :] = jnp.zeros((rows_p - blank, u_len), F32)
    v_rows[blank:rows_p, :] = jnp.zeros((rows_p - blank, v_len), F32)
    own_v.wait()
    for p in range(row_n):
        v_code[p] = encode(v_in[:, p * v_len:(p + 1) * v_len])
    pl.semaphore_wait(barrier, row_n + col_n - 2)
    v_init = send("row", row_me, row_n, lambda p: v_code.at[p], lambda k: v_all.at[row_me],
                  lambda k: init_v_send.at[k], lambda k: init_v_recv.at[k])
    own_u.wait()
    own_t = load(8, tiles_hbm, tiles)
    for p in range(col_n):
        u_code[p] = encode(u_in[:, p * u_len:(p + 1) * u_len])
    u_init = send("col", col_me, col_n, lambda p: u_code.at[p], lambda k: u_all.at[col_me],
                  lambda k: init_u_send.at[k], lambda k: init_u_recv.at[k])
    v_all[row_me] = v_code[row_me]
    u_all[col_me] = u_code[col_me]

    for copy in own_places:
        copy.wait()
    active = lax.broadcasted_iota(I32, (1, slots), 1) < count_ref[...]

    def hot_of(places, blocks, pick, put):
        hot = jnp.where(
            (lax.broadcasted_iota(I32, (blocks, slots), 0) == places) & active, 1.0, 0.0).astype(BF16)
        eye = (lax.broadcasted_iota(I32, (blocks, blocks), 0)
               == lax.broadcasted_iota(I32, (blocks, blocks), 1))
        pick[...] = lax.dot_general(hot, jnp.where(eye, 1.0, 0.0).astype(BF16), (((0,), (0,)), ((), ())),
                                    preferred_element_type=F32).astype(BF16)
        put[...] = jnp.concatenate([hot, hot, hot], axis=1)

    hot_of(rows_ref[...], row_blocks, row_pick, row_put)
    hot_of(cols_ref[...], col_blocks, col_pick, col_put)

    own_t.wait()
    unit[...] = jnp.where(lax.broadcasted_iota(I32, (tile, tile), 0) == lax.broadcasted_iota(I32, (tile, tile), 1),
                          1.0, 0.0).astype(BF16)

    def turn(g, carry):
        base = pl.multiple_of(g * 8, 8)
        for i in range(8):
            turned[base + i] = lax.dot_general(unit[...], tiles[base + i], (((1,), (1,)), ((), ())),
                                               preferred_element_type=F32).astype(BF16)
        return carry

    lax.fori_loop(0, slots // 8, turn, 0)

    row_id = lax.broadcasted_iota(I32, (rows_p, LANE), 0)
    lane_id = lax.broadcasted_iota(I32, (rows_p, LANE), 1)
    lane_row = lax.broadcasted_iota(I32, (1, LANE), 1)
    eye = row_id == lane_id

    def to_row(column):
        return jnp.sum(jnp.where(eye, column, 0.0), axis=0, keepdims=True)

    def add_up(buf, n):
        parts = [buf[i] for i in range(n)]
        while len(parts) > 1:
            parts = [parts[i] + parts[i + 1] if i + 1 < len(parts) else parts[i]
                     for i in range(0, len(parts), 2)]
        return parts[0]

    def sum_all_devices(row, index, between=lambda: None):
        if direct:
            me = row_me * col_n + col_me
            buf = sum_all.at[index]
            buf[pl.ds(me, 1), :] = row
            pairs = [(a, b) for a in range(row_n) for b in range(col_n) if a or b]
            pairs.sort(key=lambda p: -(p[0] // 2 + bin(p[1]).count("1")))
            copies, sends = [], send_sems()
            for k, (a, b) in enumerate(pairs):
                where = {"row": partner(row_me, a, row_n), "col": partner(col_me, b, col_n)}
                copy = pltpu.make_async_remote_copy(
                    src_ref=buf.at[pl.ds(me, 1)], dst_ref=buf.at[pl.ds(me, 1)], send_sem=sends(k),
                    recv_sem=sum_all_sem.at[index, 0], device_id=where,
                    device_id_type=pl.DeviceIdType.MESH)
                copy.start()
                copies.append(copy)
            rest = buf.at[pl.ds(0, row_n * col_n - 1)]
            flight(copies, between, pltpu.make_async_copy(rest, rest, sum_all_sem.at[index, 0]))
            return jnp.sum(buf[...], axis=0, keepdims=True)
        buf = sum_col.at[index]
        buf[pl.ds(col_me, 1), :] = row
        flight(send("col", col_me, col_n, lambda p: buf.at[pl.ds(col_me, 1)], lambda k: buf.at[pl.ds(col_me, 1)],
                    send_sems(), lambda k: sum_col_sem.at[index, k]), between)
        row = jnp.sum(buf[...], axis=0, keepdims=True)
        buf = sum_row.at[index]
        buf[pl.ds(row_me, 1), :] = row
        flight(send("row", row_me, row_n, lambda p: buf.at[pl.ds(row_me, 1)], lambda k: buf.at[pl.ds(row_me, 1)],
                    send_sems(), lambda k: sum_row_sem.at[index, k]))
        return jnp.sum(buf[...], axis=0, keepdims=True)

    def coef(basis, place):
        acc = jnp.zeros((rows_p, LANE), F32)
        for j in range(basis.shape[1] // LANE):
            at = slice(j * LANE, (j + 1) * LANE)
            acc = acc + basis[:, at] * basis[place:place + 1, at]
        return to_row(jnp.sum(acc, axis=1, keepdims=True))

    def tables(gram, place):
        small = lax.dot_general(gram, gram, (((1,), (1,)), ((), ())), precision=HIGH, preferred_element_type=F32)
        square = jnp.concatenate([small, jnp.zeros((rows_p, LANE - rows_p), F32)], axis=1)
        one = jnp.where(eye & (row_id < place), 1.0, 0.0)
        return 2.0 * one - gram, one - (2.0 * gram - square), one

    def solve(row, place, table):
        both, left, one = table
        got = jnp.where(lane_row < place, row, 0.0)
        square = jnp.sum(jnp.where(lane_row == place, row, 0.0), axis=1, keepdims=True)
        column = jnp.sum(both * got, axis=1, keepdims=True)
        square = square - jnp.sum(column * jnp.sum((one + left) * got, axis=1, keepdims=True), axis=0, keepdims=True)
        scale = jnp.sqrt(square + 1e-06)
        return got, left, square, column, scale, 1.0 / scale

    def apply(basis, vec, place, found):
        column, inverse = found[3], found[5]
        spread = jnp.broadcast_to(jnp.where(row_id[:, 0:1] == place, 1.0, -column), (rows_p, LANE))
        for j in range(basis.shape[1] // LANE):
            at = slice(j * LANE, (j + 1) * LANE)
            s, h = j * LANE // tile, j * LANE % tile
            vec[s:s + 1, h:h + LANE] = jnp.sum(spread * basis[:, at], axis=0, keepdims=True)
        return vec[...] * inverse

    def grow_basis(basis, place, found, out, gram):
        got, left, square, column, scale, inverse = found
        for s in range(out.shape[0]):
            basis[place:place + 1, s * tile:(s + 1) * tile] = out[s:s + 1, :]
        if gram is None:
            return None
        cross = jnp.sum(left * got, axis=1, keepdims=True) * inverse
        grown = jnp.where(row_id == place, to_row(cross), gram)
        grown = jnp.where(lane_id == place, cross, grown)
        corner = (row_id == place) & (lane_id == place)
        return jnp.where(corner, square / (scale * scale), grown)

    def apply_full(step, found):
        column, inverse = found[3], found[5]
        spread = jnp.broadcast_to(jnp.where(row_id[0:keep_p, 0:1] < keep_n, -column[0:keep_p], 0.0), (keep_p, LANE))
        for q in range(col_n):
            for j in range(u_len // LANE):
                at = slice(j * LANE, (j + 1) * LANE)
                s, h = q * u_sub + j * LANE // tile, j * LANE % tile
                full_y[s:s + 1, h:h + LANE] = jnp.sum(spread * full_u[q, :, at], axis=0, keepdims=True)
        x = jnp.concatenate([x_full[step, q] for q in range(col_n)], axis=0)
        for old in range(step):
            before = jnp.concatenate([new_full[old, q] for q in range(col_n)], axis=0)
            x = x - column[keep_n + old:keep_n + old + 1, 0:1] * before
        return (x + full_y[...]) * inverse

    def joined(gathered, n):
        return jnp.concatenate([gathered[i].astype(F32) for i in range(n)], axis=0).astype(BF16)

    def matvec(full, pick, put, blocks):
        picked[...] = jnp.dot(pick[...], full, preferred_element_type=F32)
        sub = lax.broadcasted_iota(I32, (8, tile), 0)
        for g in range(slots // 8):
            left = picked[g * 8:(g + 1) * 8, :].astype(BF16)
            acc = jnp.zeros((8, tile), F32)
            for i in range(8):
                res = jnp.dot(left, blocks[g * 8 + i], preferred_element_type=F32)
                acc = jnp.where(sub == i, res, acc)
            products[g * 8:(g + 1) * 8, :] = acc
        full = products[...]
        high = full.astype(BF16)
        rest = full - high.astype(F32)
        middle = rest.astype(BF16)
        low = (rest - middle.astype(F32)).astype(BF16)
        return jnp.dot(put[...], jnp.concatenate([high, middle, low], axis=0), preferred_element_type=F32)

    def gather(axis, me, n, own, buf, sems, between):
        buf[me] = own.astype(BF16)
        flight(send(axis, me, n, lambda p: buf.at[me], lambda k: buf.at[me], send_sems(), sems), between)

    def scatter(axis, me, n, value, basis, place, sub, parts, recv, sems, between=lambda: None):
        for i in range(n):
            parts[i] = value[i * sub:(i + 1) * sub, :]
        flight(send(axis, me, n, lambda p: parts.at[p], lambda k: recv.at[k], send_sems(), sems), between)
        total = parts[me]
        for k in range(1, n):
            total = total + recv[k]
        for s in range(sub):
            basis[place:place + 1, s * tile:(s + 1) * tile] = total[s:s + 1, :]
        return total

    def kept(keep, source, target):
        factor = keep[...]
        high = factor.astype(BF16)
        low = (factor - high.astype(F32)).astype(BF16)
        left = jnp.concatenate(
            [jnp.concatenate([high, high], axis=1), jnp.concatenate([low, jnp.zeros(low.shape, BF16)], axis=1)], axis=0)
        step = min(512, target.shape[1])
        for j in range(target.shape[1] // step):
            at = slice(j * step, (j + 1) * step)
            data = jnp.concatenate([decode(source[i, :, at]) for i in range(source.shape[0])], axis=0)
            top = data.astype(BF16)
            rest = (data - top.astype(F32)).astype(BF16)
            both = jnp.dot(left, jnp.concatenate([top, rest], axis=0), preferred_element_type=F32)
            target[0:keep_p, at] = both[0:keep_p] + both[keep_p:2 * keep_p]

    def half_gram(basis):
        wide = basis[...]
        small = lax.dot_general(wide, wide, (((1,), (1,)), ((), ())), precision=HIGH, preferred_element_type=F32)
        full = jnp.concatenate([small, jnp.zeros((rows_p, LANE - rows_p), F32)], axis=1)
        packed = jnp.zeros((8, LANE), F32)
        for at, shift in starts:
            block = jnp.where((lane_id[0:8] >= at) & (lane_id[0:8] < real), full[at:at + 8], 0.0)
            packed = packed + (pltpu.roll(block, shift, 1) if shift else block)
        return packed

    def unpack(packed):
        pieces = []
        for at, shift in starts:
            block = pltpu.roll(packed, LANE - shift, 1) if shift else packed
            pieces.append(jnp.where((lane_id[0:8] >= at) & (lane_id[0:8] < real), block, 0.0))
        pieces.append(jnp.zeros((LANE - 8 * len(pieces), LANE), F32))
        upper = jnp.concatenate(pieces, axis=0)
        row_block = lax.div(lax.broadcasted_iota(I32, (LANE, LANE), 0), 8)
        lane_block = lax.div(lax.broadcasted_iota(I32, (LANE, LANE), 1), 8)
        full = upper + jnp.transpose(jnp.where(lane_block > row_block, upper, 0.0))
        return full[0:rows_p]

    def row_spread(buf, value, index):
        buf[row_me] = value
        return send("row", row_me, row_n, lambda p: buf.at[row_me], lambda k: buf.at[row_me],
                    lambda k: gram_send.at[index, k], lambda k: gram_recv.at[index, k])

    def col_spread(buf, value, index):
        buf[col_me] = value
        return send("col", col_me, col_n, lambda p: buf.at[col_me], lambda k: buf.at[col_me],
                    lambda k: gram_send.at[index, k], lambda k: gram_recv.at[index, k])

    early = []
    own_next.wait()
    own_keep_v.wait()
    own_keep_u.wait()
    v_rows[keep_n:keep_n + 1, :] = v_first[...]
    finish(v_init)
    kept(keep_v, v_all, v_rows)
    v_copies = col_spread(gram_v_col, half_gram(v_rows), 0)
    finish(u_init)
    kept(keep_u, u_all, u_rows)
    u_copies = col_spread(gram_u_col, half_gram(u_rows), 2)
    full_copies = []
    cut = u_len * 3 // 4

    def full_spread(index, a, b):
        full_copies.extend(send(
            "col", col_me, col_n, lambda p: full_code.at[col_me, :, a:b], lambda k: full_code.at[col_me, :, a:b],
            lambda k: full_send.at[index, k], lambda k: full_recv.at[index, k]))

    full_code[col_me] = encode(u_rows[0:keep_p, :], wide_coarse)
    full_spread(0, 0, cut)
    finish(v_copies)
    v_copies = row_spread(gram_v_row, add_up(gram_v_col, col_n), 1)
    finish(u_copies)
    u_copies = row_spread(gram_u_row, add_up(gram_u_col, col_n), 3)
    finish(v_copies)
    wide = unpack(add_up(gram_v_row, row_n)) * (1.0 / v_total)
    first_row = wide[keep_n:keep_n + 1, :]
    gram_v = jnp.where((row_id < keep_n) & (lane_id < keep_n), wide, 0.0)
    found = solve(first_row, keep_n, tables(gram_v, keep_n))
    out = apply(v_rows, v_vec, keep_n, found)

    state = {"v": gram_v, "u": None}

    def write_kept():
        if blank:
            early.append(load(11, u_rows.at[0:blank], u_out.at[0:blank]))
            early.append(load(12, v_rows.at[0:blank], v_out.at[0:blank]))


    def between_v(place, found, out, step):
        def run():
            state["v"] = grow_basis(v_rows, place, found, out, state["v"])
            state["v_table"] = tables(state["v"], place + 1)
            if step == 1:
                finish(full_copies)
                for q in range(col_n):
                    full_u[q] = decode(full_code[q], wide_coarse)
                full_u[col_me] = u_rows[0:keep_p, :]
        return run

    def grow_u(place, found, out, step):
        if step + 1 < STEPS:
            state["u"] = grow_basis(u_rows, place, found, out, state["u"])
            state["u_table"] = tables(state["u"], place + 1)
        else:
            grow_basis(u_rows, place, found, out, None)

    def gram_end():
        finish(u_copies)
        gram_u = unpack(add_up(gram_u_row, row_n)) * (1.0 / u_total)
        state["u"] = jnp.where((row_id < keep_n) & (lane_id < keep_n), gram_u, 0.0)
        state["u_table"] = tables(state["u"], keep_n)

    def between_u(place, grow, step):
        def run():
            if step + 1 < STEPS:
                state["u"] = grow(state["u"])
                state["u_table"] = tables(state["u"], place + 1)
            else:
                grow(None)
        return run

    def between_u(place, found, out, step):
        return lambda: grow_u(place, found, out, step)

    def share_new(out):
        def run():
            full_spread(1, cut, u_len)
            new_full[0, col_me] = out
            full_copies.extend(send(
                "col", col_me, col_n, lambda p: new_full.at[0, col_me], lambda k: new_full.at[0, col_me],
                lambda k: xf_send.at[0, k], lambda k: xf_recv.at[0, k]))
        return run

    def late_u(place, found, step):
        return lambda: grow_u(place, found, apply(u_rows, u_vec, place, found), step)

    alphas, betas = [], []
    for step in range(STEPS):
        u_place, v_place = keep_n + step, keep_n + 1 + step
        gather("row", row_me, row_n, out, v_gather.at[step], lambda k: vg_sem.at[step, k],
               between_v(v_place - 1, found, out, step))
        partial = matvec(joined(v_gather.at[step], row_n), col_pick, row_put, turned)
        total = scatter("col", col_me, col_n, partial, u_rows, u_place, u_sub, u_parts, u_recv.at[step],
                        lambda k: ur_sem.at[step, k],
                        gram_end if step == 0 else write_kept if step == 1 else lambda: None)
        if step == 0:
            row = sum_all_devices(coef(u_rows, u_place), 2 * step) * (1.0 / u_total)
            found = solve(row, u_place, state["u_table"])
            out = apply(u_rows, u_vec, u_place, found)
            gather("col", col_me, col_n, out, u_gather.at[step], lambda k: ug_sem.at[step, k],
                   between_u(u_place, found, out, step))
            full, between = joined(u_gather.at[step], col_n), share_new(out) if STEPS > 1 else lambda: None
        else:
            x_copies = []

            def share_x(step=step, total=total):
                x_full[step, col_me] = total
                x_copies.extend(send(
                    "col", col_me, col_n, lambda p: x_full.at[step, col_me], lambda k: x_full.at[step, col_me],
                    lambda k: xf_send.at[step, k], lambda k: xf_recv.at[step, k]))

            row = sum_all_devices(coef(u_rows, u_place), 2 * step, share_x) * (1.0 / u_total)
            found = solve(row, u_place, state["u_table"])
            finish(x_copies)
            wide = apply_full(step, found)
            if step + 1 < STEPS:
                for q in range(col_n):
                    new_full[step, q] = wide[q * u_sub:(q + 1) * u_sub]
            full, between = wide.astype(BF16), late_u(u_place, found, step)
        alphas.append(found[4])
        partial = matvec(full, row_pick, col_put, tiles)
        scatter("row", row_me, row_n, partial, v_rows, v_place, v_sub, v_parts, v_recv.at[step],
                lambda k: vr_sem.at[step, k], between)
        row = sum_all_devices(coef(v_rows, v_place), 2 * step + 1) * (1.0 / v_total)
        found = solve(row, v_place, state["v_table"])
        out = apply(v_rows, v_vec, v_place, found)
        betas.append(found[4])
    grow_basis(v_rows, keep_n + STEPS, found, out, None)
    place_r = lax.broadcasted_iota(I32, (8, LANE), 0)
    place_l = lax.broadcasted_iota(I32, (8, LANE), 1)
    result = jnp.zeros((8, LANE), F32)
    for step in range(STEPS):
        result = jnp.where((place_r == 0) & (place_l == step), alphas[step], result)
        result = jnp.where((place_r == 1) & (place_l == step), betas[step], result)
    bi_out[...] = result
    copies = [load(9, u_rows.at[blank:rows_p], u_out.at[blank:rows_p]),
              load(10, v_rows.at[blank:rows_p], v_out.at[blank:rows_p])]
    for copy in sent:
        copy.wait_send()
    finish(early)
    finish(copies)


def close(u_ref, v_ref, bi_ref, u_out, v_out, bi_out, u_in, v_in, bi_in, u_fit, v_fit, bi_fit, sem):
    pieces = [(bi_ref, bi_in, bi_fit, bi_out, None)]
    for here, inside, fit, there, n in ((u_ref, u_in, u_fit, u_out, 4), (v_ref, v_in, v_fit, v_out, 2)):
        step = here.shape[1] // n
        pieces += [(here, inside, fit, there, slice(i * step, (i + 1) * step)) for i in range(n)]
    loads = []
    for i, (here, inside, fit, there, at) in enumerate(pieces):
        source, target = (here, inside) if at is None else (here.at[:, at], inside.at[:, at])
        loads.append(pltpu.make_async_copy(source, target, sem.at[0, i]))
        loads[-1].start()
    stores = []
    for i, (here, inside, fit, there, at) in enumerate(pieces):
        loads[i].wait()
        if at is None:
            fit[...] = inside[0:fit.shape[0], 0:fit.shape[1]]
            store = pltpu.make_async_copy(fit, there, sem.at[1, i])
        else:
            fit[:, at] = inside[0:fit.shape[0], at]
            store = pltpu.make_async_copy(fit.at[:, at], there.at[:, at], sem.at[1, i])
        store.start()
        stores.append(store)
    for store in stores:
        store.wait()


def per_device(
    u_start, v_start, keep_u, keep_v, v_next, tile_blocks, tile_rows, tile_cols, tile_count
):
    row_n = lax.axis_size("row")
    col_n = lax.axis_size("col")
    u_here, v_here = u_start.shape[0], v_start.shape[0]
    basis, keep_n = keep_u.shape
    u_len = u_start.shape[1] // col_n
    v_len = v_start.shape[1] // row_n
    slots, tile = tile_blocks.shape[0], tile_blocks.shape[1]
    rows_p = -(-(keep_n + 1 + STEPS) // 8) * 8
    keep_p = -(-keep_n // 8) * 8
    assert rows_p <= LANE
    pad = ((0, keep_p - keep_n), (0, 0))
    sums = 2 * STEPS
    total_n = row_n * col_n
    direct_n = total_n if total_n <= DIRECT else 1
    staged = 1 if total_n <= DIRECT else sums
    dma = pltpu.SemaphoreType.DMA
    vmem = pl.BlockSpec(memory_space=pltpu.VMEM)
    hbm = pl.BlockSpec(memory_space=pltpu.HBM)
    u_sub, v_sub = u_len // tile, v_len // tile
    row_blocks, col_blocks = col_n * u_sub, row_n * v_sub
    most = max(row_n, col_n)
    padded = pl.pallas_call(
        functools.partial(kernel, row_n, col_n, keep_n),
        out_shape=(
            jax.ShapeDtypeStruct((rows_p, u_len), F32),
            jax.ShapeDtypeStruct((rows_p, v_len), F32),
            jax.ShapeDtypeStruct((8, LANE), F32),
        ),
        in_specs=[hbm] * 9,
        out_specs=(hbm, hbm, vmem),
        scratch_shapes=[
            pltpu.VMEM(u_start.shape, F32),
            pltpu.VMEM(v_start.shape, F32),
            pltpu.VMEM((col_n, u_here, u_len), I16),
            pltpu.VMEM((row_n, v_here, v_len), I16),
            pltpu.VMEM((col_n, u_here, u_len), I16),
            pltpu.VMEM((row_n, v_here, v_len), I16),
            pltpu.VMEM(tile_blocks.shape, BF16),
            pltpu.VMEM(tile_blocks.shape, BF16),
            pltpu.VMEM((tile, tile), BF16),
            pltpu.VMEM((keep_p, basis), F32),
            pltpu.VMEM((keep_p, basis), F32),
            pltpu.VMEM((1, v_len), F32),
            pltpu.VMEM((1, slots), I32),
            pltpu.VMEM((1, slots), I32),
            pltpu.VMEM((1, 1), I32),
            pltpu.VMEM((rows_p, u_len), F32),
            pltpu.VMEM((rows_p, v_len), F32),
            pltpu.VMEM((u_sub, tile), F32),
            pltpu.VMEM((v_sub, tile), F32),
            pltpu.VMEM((col_n, 8, LANE), F32),
            pltpu.VMEM((row_n, 8, LANE), F32),
            pltpu.VMEM((col_n, 8, LANE), F32),
            pltpu.VMEM((row_n, 8, LANE), F32),
            pltpu.VMEM((staged, col_n, LANE), F32),
            pltpu.VMEM((staged, row_n, LANE), F32),
            pltpu.VMEM((sums, direct_n, LANE), F32),
            pltpu.VMEM((STEPS, row_n, v_sub, tile), BF16),
            pltpu.VMEM((STEPS, col_n, u_sub, tile), BF16),
            pltpu.VMEM((col_n, u_sub, tile), F32),
            pltpu.VMEM((row_n, v_sub, tile), F32),
            pltpu.VMEM((STEPS, col_n, u_sub, tile), F32),
            pltpu.VMEM((STEPS, row_n, v_sub, tile), F32),
            pltpu.VMEM((slots, row_blocks), BF16),
            pltpu.VMEM((slots, col_blocks), BF16),
            pltpu.VMEM((row_blocks, 3 * slots), BF16),
            pltpu.VMEM((col_blocks, 3 * slots), BF16),
            pltpu.VMEM((slots, tile), F32),
            pltpu.VMEM((slots, tile), F32),
            pltpu.VMEM((col_n, keep_p, u_len), I16),
            pltpu.VMEM((col_n, keep_p, u_len), F32),
            pltpu.VMEM((row_blocks, tile), F32),
            pltpu.VMEM((STEPS, col_n, u_sub, tile), F32),
            pltpu.VMEM((STEPS, col_n, u_sub, tile), F32),
            dma((13,)),
            dma((col_n,)),
            dma((col_n,)),
            dma((row_n,)),
            dma((row_n,)),
            dma((2, max(most, direct_n))),
            dma((4, most)),
            dma((4, most)),
            dma((staged, col_n)),
            dma((staged, row_n)),
            dma((sums, direct_n)),
            dma((STEPS, row_n)),
            dma((STEPS, col_n)),
            dma((STEPS, col_n)),
            dma((STEPS, row_n)),
            dma((2, col_n)),
            dma((2, col_n)),
            dma((STEPS, col_n)),
            dma((STEPS, col_n)),
        ],
        compiler_params=pltpu.CompilerParams(
            collective_id=0, has_side_effects=True, vmem_limit_bytes=62 * 1024 * 1024
        ),
    )(
        u_start, v_start, jnp.pad(keep_u.T, pad), jnp.pad(keep_v.T, pad), v_next.reshape(1, -1), tile_blocks,
        tile_rows.reshape(1, -1), tile_cols.reshape(1, -1), tile_count.reshape(1, 1),
    )
    final = (
        jax.ShapeDtypeStruct((keep_n + STEPS, u_len), F32),
        jax.ShapeDtypeStruct((keep_n + 1 + STEPS, v_len), F32),
        jax.ShapeDtypeStruct((2, STEPS), F32),
    )
    return pl.pallas_call(
        close,
        out_shape=final,
        in_specs=[hbm] * 3,
        out_specs=(hbm, hbm, hbm),
        scratch_shapes=[pltpu.VMEM(x.shape, F32) for x in (*padded, *final)] + [dma((2, 7))],
        compiler_params=pltpu.CompilerParams(vmem_limit_bytes=62 * 1024 * 1024),
    )(*padded)


def solution(mesh):
    return jax.shard_map(
        per_device,
        mesh=mesh,
        in_specs=(
            P("col", "row"),
            P("row", "col"),
            P(),
            P(),
            P(("col", "row")),
            P(("row", "col"), None, None),
            P(("row", "col")),
            P(("row", "col")),
            P(("row", "col")),
        ),
        out_specs=(P(None, ("row", "col")), P(None, ("col", "row")), P()),
        check_vma=False,
    )
```
